32 devices in a mesh: dev: 8 (over z, y), rep: 4 (over x, core).
Axes of the slice: x: 2, y: 2, z: 4, core: 2. Of those that a mesh axis runs over, the one named last changes fastest.
Arguments:
- features: bfloat16 [32768, 256], P(('dev', 'rep')), may hold values from -6 to 6
- history: bfloat16 [32768, 256], P(('dev', 'rep')), may hold values from -6 to 6
- new_owner: int32 [32, 8], P(('dev', 'rep')), may hold values from 0 to 7, as said below
- pull_rows: int32 [32768], P(('dev', 'rep')), may hold values from 0 to 1023
- occupancy: int32 [256, 16], P(('dev', 'rep')), may hold values from 0 to 1, as said below
- adj_local: bfloat16 [32768, 1024], P(('dev', 'rep')), may hold values from -0.125 to 0.125
- adj_boundary: bfloat16 [32768, 1024], P(('dev', 'rep')), may hold values from -0.125 to 0.125
- w_first: bfloat16 [256, 256], replicated, may hold values from -0.375 to 0.375
- bias_first: float32 [256], replicated, may hold values from -3 to 3
- w_second: bfloat16 [256, 256], replicated, may hold values from -0.375 to 0.375
- cotangent: bfloat16 [32768, 256], P(('dev', 'rep')), may hold values from -6 to 6
Outputs:
- hidden: bfloat16 [32768, 256], P(('dev', 'rep'))
- output: bfloat16 [32768, 256], P(('dev', 'rep'))
- w_second_grad: float32 [256, 256], replicated
The draws below stay inside these ranges and needn't reach their ends.
Inputs may be any that keep to these rules, and one draw needn't show every extreme that they name: Each row of new_owner is a permutation of 0 to 7. `occupancy`: tile flags of 0 or 1.
All inputs are finite; a program needn't handle non-finite values.
Results may differ from the reference program's by a relative error of at most 0.0061.
Values may be sent and summed in bfloat16 or wider, within the bound.
A program may use at most 64 MiB of HBM per device.

```python
import jax
import jax.numpy as jnp
from jax import lax

F = 256
ROWS_DEV = 1024
PULL_DEV = 1024
NODES = 32768
N_DEV = 8
N_REP = 4


def draw_new_owner(key, part):
    keys = jax.random.split(jax.random.fold_in(key, 11), N_DEV * N_REP)

    def shuffle(single):
        return jax.random.permutation(single, N_DEV)
    return jax.vmap(shuffle)(keys).astype(jnp.int32)


def draw_occupancy(key, part):
    tile_rows = ROWS_DEV // 128
    tile_cols = (ROWS_DEV + PULL_DEV) // 128
    total = N_DEV * N_REP
    first, second = jax.random.split(jax.random.fold_in(key, 23))
    level = jax.random.randint(first, (total, 1, 1), 1, 5)
    rolled = jax.random.randint(second, (total, tile_rows, tile_cols), 0, 4)
    return (rolled < level).astype(jnp.int32).reshape(total * tile_rows, tile_cols)


def set_ends(entries, stream_key, smallest, top_value):
    spot = [jax.random.randint(jax.random.fold_in(stream_key, axis), (), 0, length) for axis, length in enumerate(entries.shape)]
    longest = entries.shape.index(max(entries.shape))
    next_to = spot[:longest] + [(spot[longest] + 1) % entries.shape[longest]] + spot[longest + 1:]
    return entries.at[tuple(spot)].set(smallest).at[tuple(next_to)].set(top_value)


def with_spikes(values, rng, source, target, shards_of, factor):
    def block_of(dim):
        return (jnp.arange(values.shape[dim]) // (values.shape[dim] // shards_of)).reshape((-1,) + (1,) * (values.ndim - 1 - dim))

    first = jax.random.permutation(rng, shards_of)[block_of(target)]
    other_side = (block_of(target) + shards_of // 2) % shards_of
    return jnp.where((block_of(source) == first) | (block_of(source) == other_side), factor * values, values)


def block_scale(stream_key, dims, shards, low, high):
    def one(dim, shards_of):
        draws = jax.random.uniform(jax.random.fold_in(jax.random.fold_in(stream_key, 6), dim), (shards_of,), jnp.float32, low / len(shards), high / len(shards))
        return jnp.repeat(jnp.exp(draws), dims[dim] // shards_of).reshape((-1,) + (1,) * (len(dims) - dim - 1))

    loudness = one(*shards[0])
    for cut in shards[1:]:
        loudness = loudness * one(*cut)
    return loudness


def bell_draw(stream_key, dims, scale, limit, cuts=(), kind=jnp.bfloat16):
    loudness = block_scale(stream_key, dims, cuts, -0.22, 0.18) if cuts else 1.0
    values = jax.random.normal(stream_key, dims, jnp.float32) * scale * loudness
    return jnp.minimum(jnp.maximum(values, -limit), limit).astype(kind)


def gaussian_with(stream_key, extent, scale, bound, cuts, heavy, kind=jnp.bfloat16):
    array = scale * jax.random.normal(stream_key, extent, jnp.float32)
    if cuts:
        array = array * block_scale(stream_key, extent, cuts, -0.22, 0.18)
    return jnp.clip(with_spikes(array, jax.random.fold_in(stream_key, 3), *heavy), -bound, bound).astype(kind)


def setup_inputs(seed: int = 0) -> dict:
    splits = jax.random.split(jax.random.key(seed), 12)
    features = bell_draw(splits[0], (NODES, F), 1.0, 6.0, ((0, 32),))
    history = bell_draw(splits[1], (NODES, F), 1.0, 6.0, ((0, 32),))
    new_owner = draw_new_owner(jax.random.fold_in(splits[11], 71), 0)
    pull_rows = set_ends(jax.random.randint(splits[3], (N_DEV * N_REP * PULL_DEV,), 0, ROWS_DEV), jax.random.fold_in(splits[3], 1), 0, ROWS_DEV - 1).astype(jnp.int32)
    occupancy = draw_occupancy(jax.random.fold_in(splits[11], 71), 0)
    adj_local = bell_draw(splits[5], (NODES, ROWS_DEV), (ROWS_DEV + PULL_DEV) ** -0.5, 0.125, ((0, 32),))
    adj_boundary = bell_draw(splits[6], (NODES, PULL_DEV), (ROWS_DEV + PULL_DEV) ** -0.5, 0.125, ((0, 32),))
    w_first = bell_draw(splits[7], (F, F), F ** -0.5, 0.375)
    bias_first = bell_draw(splits[8], (F,), 0.5, 3.0, (), jnp.float32)
    w_second = bell_draw(splits[9], (F, F), F ** -0.5, 0.375)
    cotangent = gaussian_with(splits[10], (NODES, F), 1.0, 6.0, ((0, 32),), (0, 1, 32, 2.75))
    return dict(features=features, history=history, new_owner=new_owner, pull_rows=pull_rows, occupancy=occupancy, adj_local=adj_local, adj_boundary=adj_boundary, w_first=w_first, bias_first=bias_first, w_second=w_second, cotangent=cotangent)


def expand(occupied):
    return jnp.repeat(jnp.repeat(occupied, 128, axis=-2), 128, axis=-1).astype(jnp.bfloat16)


def reference(features, history, new_owner, pull_rows, occupancy, adj_local, adj_boundary, w_first, bias_first, w_second, cotangent):
    peer_count = N_DEV
    copies = N_REP
    height = ROWS_DEV
    breadth = F
    cluster = height // peer_count
    pulled = PULL_DEV
    per_peer = pulled // peer_count
    indices = jnp.arange(peer_count, dtype=jnp.int32)
    routes = new_owner.reshape(peer_count, copies, peer_count)
    matches = (routes[:, :, :, None] == indices).astype(jnp.int32)
    inverse = jnp.sum(matches * indices[:, None], axis=2).astype(jnp.int32)

    def migrate(values):
        blocks = values.reshape(peer_count, copies, peer_count, cluster, breadth)
        where_from = jnp.broadcast_to(inverse[:, :, :, None, None], blocks.shape)
        arrived = jnp.take_along_axis(blocks, where_from, axis=2)
        return arrived.transpose(2, 1, 0, 3, 4).reshape(peer_count, copies, height, breadth)

    own_x = migrate(features)
    own_h = migrate(history)
    wanted = pull_rows.reshape(peer_count, copies, pulled)
    owners = jnp.arange(pulled, dtype=jnp.int32) // per_peer
    flat_rows = (owners[None, None, :] * height + wanted).astype(jnp.int32)
    replica_ids = jnp.arange(copies, dtype=jnp.int32)[None, :, None]

    def fetch_remote(values):
        spread = values.transpose(1, 0, 2, 3).reshape(copies, peer_count * height, breadth)
        return spread[replica_ids, flat_rows]

    def scatter(partial_value):
        summed = jnp.zeros((copies, peer_count * height, breadth), jnp.float32)
        summed = summed.at[replica_ids, flat_rows].add(partial_value.astype(jnp.float32))
        summed = summed.reshape(copies, peer_count, height, breadth).transpose(1, 0, 2, 3)
        return summed.reshape(peer_count * copies * height, breadth)

    tile_mask = occupancy.reshape(peer_count * copies, height // 128, (height + pulled) // 128)
    local_adj = adj_local.reshape(peer_count * copies, height, height)
    edge_adj = adj_boundary.reshape(peer_count * copies, height, pulled)

    def layer_terms(owned, remote):
        def device(operands):
            owned_rows, theirs, local_tile, edge_tile, flags = operands
            full_mask = expand(flags)
            local_tile = local_tile * full_mask[:, :height]
            edge_tile = edge_tile * full_mask[:, height:]
            summed = jnp.dot(local_tile, owned_rows, preferred_element_type=jnp.float32)
            summed = summed + jnp.dot(edge_tile, theirs, preferred_element_type=jnp.float32)
            partial_value = lax.dot_general(edge_tile, owned_rows, (((0,), (0,)), ((), ())), preferred_element_type=jnp.float32)
            return summed, partial_value.astype(jnp.bfloat16)

        summed, partial_value = lax.map(device, (owned.reshape(-1, height, breadth), remote.reshape(-1, pulled, breadth), local_adj, edge_adj, tile_mask))
        return summed.reshape(-1, breadth), partial_value.reshape(peer_count, copies, pulled, breadth)

    summed_one, partial_one = layer_terms(own_x, fetch_remote(own_x))
    aggregate_one = (summed_one + scatter(partial_one)).astype(jnp.bfloat16)
    hidden = jnp.maximum(jnp.dot(aggregate_one, w_first, preferred_element_type=jnp.float32) + bias_first, 0.0).astype(jnp.bfloat16)
    summed_two, partial_two = layer_terms(hidden.reshape(peer_count, copies, height, breadth), fetch_remote(own_h))
    aggregate_two = (summed_two + scatter(partial_two)).astype(jnp.bfloat16)
    output = jnp.dot(aggregate_two, w_second, preferred_element_type=jnp.float32).astype(jnp.bfloat16)
    gradient = lax.dot_general(aggregate_two, cotangent, (((0,), (0,)), ((), ())), preferred_element_type=jnp.float32)
    return hidden, output, gradient
```

```python
import functools

import jax
import jax.numpy as jnp
from jax import lax
from jax.experimental import pallas as pl
from jax.experimental.pallas import tpu as pltpu
from jax.sharding import PartitionSpec as P

MESH = pl.DeviceIdType.MESH
F32 = jnp.float32
BF16 = jnp.bfloat16
ASK, MOVE_X, MOVE_H, FAR_X, FAR_H, PUSH_ONE, PUSH_TWO = range(7)


def step_kernel(
    n,
    reps,
    inner,
    features_hbm,
    history_hbm,
    new_owner_hbm,
    pulls_hbm,
    occupancy_hbm,
    adj_local_hbm,
    adj_edge_hbm,
    w_first_hbm,
    bias_first_hbm,
    w_second_hbm,
    cotangent_hbm,
    hidden,
    output_out,
    grad_out,
    features,
    history,
    new_owner,
    pulls,
    occupancy,
    w_first,
    bias_first,
    w_second,
    local,
    edge,
    edge_t,
    cotangent,
    asked,
    pick,
    pick_t,
    send_x,
    send_h,
    own_x,
    own_h,
    send_far_x,
    send_far_h,
    far_x,
    far_h,
    send_one,
    send_two,
    push_one,
    push_two,
    acc,
    agg,
    grad_mine,
    grad_near,
    strip_mine,
    strip_far,
    total_mine,
    grad_all,
    load_sem,
    send_sem,
    recv_sem,
    near_send,
    near_recv,
    far_send,
    far_recv,
):
    me = lax.axis_index("dev")
    my_rep = lax.axis_index("rep")
    height, breadth = features.shape
    cluster = height // n
    per_peer = pulls.shape[2]
    pulled = n * per_peer
    tile = height // occupancy.shape[0]
    band = min(256, height)

    def peer(off):
        return lax.rem(me + off, n)

    def rep_peer(off):
        return lax.rem(my_rep + off, reps)

    everyone = inner * reps
    outer = n // inner
    line = me // inner
    spot = lax.rem(me, inner) * reps + my_rep

    def near(off):
        return lax.rem(spot + off, everyone)

    def near_id(at):
        return {"dev": line * inner + at // reps, "rep": lax.rem(at, reps)}

    def far(off):
        return lax.rem(line + off, outer)

    def far_id(at):
        return {"dev": at * inner + lax.rem(me, inner)}

    barrier = pltpu.get_barrier_semaphore()
    for off in range(1, n):
        pl.semaphore_signal(barrier, inc=1, device_id={"dev": peer(off)}, device_id_type=MESH)
    for side in range(inner):
        for off in range(1, reps):
            pl.semaphore_signal(
                barrier,
                inc=1,
                device_id={
                    "dev": line * inner + lax.rem(me + side, inner),
                    "rep": rep_peer(off),
                },
                device_id_type=MESH,
            )

    loads = [
        pltpu.make_async_copy(source, target, load_sem.at[i])
        for i, (source, target) in enumerate(
            (
                (new_owner_hbm, new_owner),
                (features_hbm, features),
                (pulls_hbm, pulls),
                (history_hbm, history),
                (occupancy_hbm, occupancy),
                (adj_edge_hbm, edge),
                (adj_local_hbm, local),
                (w_first_hbm, w_first),
                (bias_first_hbm, bias_first),
                (w_second_hbm, w_second),
                (cotangent_hbm, cotangent),
            )
        )
    ]
    for load in loads:
        load.start()

    def cluster_for(source, owner):
        block = jnp.zeros((cluster, breadth), BF16)
        for j in range(n):
            chosen = jnp.where(new_owner[0, j] == owner, 1.0, 0.0)
            weight = jnp.full((cluster, breadth), chosen, F32).astype(BF16)
            block = block + source[j * cluster : (j + 1) * cluster, :] * weight
        return block

    def outgoing(phase, src, dst, to, slot):
        return pltpu.make_async_remote_copy(
            src_ref=src.at[to],
            dst_ref=dst.at[slot],
            send_sem=send_sem.at[phase, to],
            recv_sem=recv_sem.at[phase, slot],
            device_id={"dev": to},
            device_id_type=MESH,
        )

    def send(phase, src, dst, off):
        outgoing(phase, src, dst, peer(off), me).start()

    def receive(phase, src, dst):
        for off in range(1, n):
            other = peer(off)
            outgoing(phase, src, dst, other, other).wait_recv()

    def finish(phase, src, dst):
        for off in range(1, n):
            outgoing(phase, src, dst, peer(off), me).wait_send()

    loads[0].wait()
    loads[1].wait()
    for off in range(1, n):
        send_x[peer(off)] = cluster_for(features, peer(off))
    own_x[me] = cluster_for(features, me)
    loads[2].wait()
    pl.semaphore_wait(barrier, n - 1 + inner * (reps - 1))
    for off in range(1, n):
        send(ASK, pulls, asked, off)
    for off in range(1, n):
        send(MOVE_X, send_x, own_x, off)
    loads[3].wait()
    for off in range(1, n):
        send_h[peer(off)] = cluster_for(history, peer(off))
        send(MOVE_H, send_h, own_h, off)
    own_h[me] = cluster_for(history, me)
    asked[me] = pulls[me]

    loads[4].wait()
    loads[5].wait()
    for i in range(height // tile):
        for j in range(pulled // tile):
            kept = occupancy[i, height // tile + j].astype(F32)
            rows, cols = pl.ds(i * tile, tile), pl.ds(j * tile, tile)
            part = (edge[rows, cols].astype(F32) * kept).astype(BF16)
            edge[rows, cols] = part
            edge_t[cols, rows] = part.T
    loads[6].wait()
    for i in range(height // tile):
        for j in range(height // tile):
            kept = occupancy[i, j].astype(F32)
            rows, cols = pl.ds(i * tile, tile), pl.ds(j * tile, tile)
            local[rows, cols] = (local[rows, cols].astype(F32) * kept).astype(BF16)

    receive(ASK, pulls, asked)
    for d in range(n):
        wanted = asked[d]
        rows = lax.broadcasted_iota(jnp.int32, (height, per_peer), 0)
        pick[:, d * per_peer : (d + 1) * per_peer] = jnp.where(rows == wanted, 1.0, 0.0).astype(
            BF16
        )
        turned = jnp.broadcast_to(wanted, (per_peer, per_peer)).T
        lanes = lax.broadcasted_iota(jnp.int32, (per_peer, per_peer), 1)
        for c in range(height // per_peer):
            pick_t[d * per_peer : (d + 1) * per_peer, c * per_peer : (c + 1) * per_peer] = (
                jnp.where(turned == lanes + c * per_peer, 1.0, 0.0).astype(BF16)
            )

    def blocks_out(phase, left, right, src, dst):
        values = right[...].reshape(left.shape[1], breadth)

        def block(to):
            rows = pl.ds(pl.multiple_of(to * per_peer, per_peer), per_peer)
            return jnp.dot(left[rows, :], values, preferred_element_type=F32).astype(BF16)

        def one(off, carry):
            src[peer(off)] = block(peer(off))
            send(phase, src, dst, off)
            return carry

        lax.fori_loop(1, n, one, 0)
        dst[me] = block(me)

    def bands(body):
        def one(i, carry):
            body(pl.ds(pl.multiple_of(i * band, band), band))
            return carry

        lax.fori_loop(0, height // band, one, 0)

    def times(left, rows, right):
        values = right[...].reshape(left.shape[1], breadth)
        return jnp.dot(left[rows, :], values, preferred_element_type=F32)

    receive(MOVE_X, send_x, own_x)
    blocks_out(FAR_X, pick_t, own_x, send_far_x, far_x)
    blocks_out(PUSH_ONE, edge_t, own_x, send_one, push_one)

    def local_one(rows):
        acc[rows, :] = times(local, rows, own_x)

    bands(local_one)
    receive(MOVE_H, send_h, own_h)
    blocks_out(FAR_H, pick_t, own_h, send_far_h, far_h)
    receive(FAR_X, send_far_x, far_x)

    def edge_one(rows):
        acc[rows, :] = acc[rows, :] + times(edge, rows, far_x)

    bands(edge_one)
    receive(PUSH_ONE, send_one, push_one)

    def first(rows):
        total = (acc[rows, :] + times(pick, rows, push_one)).astype(BF16)
        value = jnp.dot(total, w_first[...], preferred_element_type=F32) + bias_first[...]
        value = jnp.maximum(value, 0.0).astype(BF16)
        hidden[rows, :] = value

    loads[7].wait()
    loads[8].wait()
    bands(first)
    blocks_out(PUSH_TWO, edge_t, hidden, send_two, push_two)

    def local_two(rows):
        acc[rows, :] = times(local, rows, hidden)

    bands(local_two)
    receive(FAR_H, send_far_h, far_h)

    def edge_two(rows):
        acc[rows, :] = acc[rows, :] + times(edge, rows, far_h)

    bands(edge_two)
    loads[9].wait()
    loads[10].wait()
    receive(PUSH_TWO, send_two, push_two)

    def second(rows):
        agg[rows, :] = (acc[rows, :] + times(pick, rows, push_two)).astype(BF16)

    bands(second)
    grad = lax.dot_general(
        agg[...], cotangent[...], (((0,), (0,)), ((), ())), preferred_element_type=F32
    )
    grad_mine[...] = grad.reshape(grad_mine.shape).astype(BF16)

    def near_copy(phase, src, dst, to, slot):
        return pltpu.make_async_remote_copy(
            src_ref=src,
            dst_ref=dst.at[slot],
            send_sem=near_send.at[phase, to],
            recv_sem=near_recv.at[phase, slot],
            device_id=near_id(to),
            device_id_type=MESH,
        )

    def far_copy(to, slot):
        return pltpu.make_async_remote_copy(
            src_ref=strip_mine,
            dst_ref=strip_far.at[slot],
            send_sem=far_send.at[to],
            recv_sem=far_recv.at[slot],
            device_id=far_id(to),
            device_id_type=MESH,
        )

    for off in range(1, everyone):
        near_copy(0, grad_mine.at[near(off)], grad_near, near(off), spot).start()

    def last(rows):
        output_out[rows, :] = jnp.dot(
            agg[rows, :], w_second[...], preferred_element_type=F32
        ).astype(BF16)

    bands(last)
    total = grad_mine[spot].astype(F32)
    for off in range(1, everyone):
        near_copy(0, grad_mine.at[near(off)], grad_near, near(off), near(off)).wait_recv()
        total = total + grad_near[near(off)].astype(F32)
    strip_mine[...] = total.astype(BF16)
    for off in range(1, outer):
        far_copy(far(off), line).start()
    strip_far[line] = strip_mine[...]
    for off in range(1, outer):
        far_copy(far(off), far(off)).wait_recv()
    total = strip_far[0].astype(F32)
    for z in range(1, outer):
        total = total + strip_far[z].astype(F32)
    total_mine[...] = total.astype(BF16)
    for off in range(1, everyone):
        near_copy(1, total_mine, grad_all, near(off), spot).start()
    grad_all[spot] = total_mine[...]
    for off in range(1, everyone):
        near_copy(1, total_mine, grad_all, near(off), near(off)).wait_recv()
    grad_out[...] = grad_all[...].astype(F32).reshape(grad_out.shape)

    finish(ASK, pulls, asked)
    finish(MOVE_X, send_x, own_x)
    finish(MOVE_H, send_h, own_h)
    finish(FAR_X, send_far_x, far_x)
    finish(FAR_H, send_far_h, far_h)
    finish(PUSH_ONE, send_one, push_one)
    finish(PUSH_TWO, send_two, push_two)
    for off in range(1, everyone):
        near_copy(0, grad_mine.at[near(off)], grad_near, near(off), spot).wait_send()
        near_copy(1, total_mine, grad_all, near(off), spot).wait_send()
    for off in range(1, outer):
        far_copy(far(off), line).wait_send()


def store_kernel(count, *refs):
    sems = refs[-1]
    copies = [
        pltpu.make_async_copy(refs[i], refs[count + i], sems.at[i]) for i in range(count)
    ]
    for copy in copies:
        copy.start()
    for copy in copies:
        copy.wait()


def store(*values):
    count = len(values)
    return pl.pallas_call(
        functools.partial(store_kernel, count),
        out_shape=tuple(jax.ShapeDtypeStruct(v.shape, v.dtype) for v in values),
        in_specs=[pl.BlockSpec(memory_space=pltpu.VMEM)] * count,
        out_specs=tuple(pl.BlockSpec(memory_space=pl.ANY) for _ in values),
        scratch_shapes=[pltpu.SemaphoreType.DMA((count,))],
        compiler_params=pltpu.CompilerParams(vmem_limit_bytes=8 * 1024 * 1024),
    )(*values)


def fused(
    features,
    history,
    new_owner,
    pull_rows,
    occupancy,
    adj_local,
    adj_boundary,
    w_first,
    bias_first,
    w_second,
    cotangent,
):
    n, reps = lax.axis_size("dev"), lax.axis_size("rep")
    height, breadth = features.shape
    cluster = height // n
    pulled = pull_rows.shape[0]
    per_peer = pulled // n
    inner = near_width(n)
    everyone = inner * reps
    part = breadth // everyone
    vmem = pl.BlockSpec(memory_space=pltpu.VMEM)
    anywhere = pl.BlockSpec(memory_space=pltpu.HBM)
    moved = pltpu.VMEM((n, cluster, breadth), BF16)
    listed = pltpu.VMEM((n, per_peer, breadth), BF16)
    square = pltpu.VMEM((everyone, part, breadth), BF16)
    strip = pltpu.VMEM((part, breadth), BF16)
    weight = pltpu.VMEM((breadth, breadth), BF16)
    nodes = pltpu.VMEM((height, breadth), BF16)
    results = pl.pallas_call(
        functools.partial(step_kernel, n, reps, inner),
        out_shape=(
            pltpu.VMEM((height, breadth), BF16),
            pltpu.VMEM((height, breadth), BF16),
            pltpu.VMEM((breadth, breadth), F32),
        ),
        in_specs=[anywhere] * 11,
        out_specs=(vmem, vmem, vmem),
        scratch_shapes=[
            nodes,
            nodes,
            pltpu.SMEM(new_owner.shape, jnp.int32),
            pltpu.VMEM((n, 1, per_peer), jnp.int32),
            pltpu.SMEM(occupancy.shape, jnp.int32),
            weight,
            pltpu.VMEM((1, breadth), F32),
            weight,
            pltpu.VMEM((height, height), BF16),
            pltpu.VMEM((height, pulled), BF16),
            pltpu.VMEM((pulled, height), BF16),
            nodes,
            pltpu.VMEM((n, 1, per_peer), jnp.int32),
            pltpu.VMEM((height, pulled), BF16),
            pltpu.VMEM((pulled, height), BF16),
            moved,
            moved,
            moved,
            moved,
            listed,
            listed,
            listed,
            listed,
            listed,
            listed,
            listed,
            listed,
            pltpu.VMEM((height, breadth), F32),
            nodes,
            square,
            square,
            strip,
            pltpu.VMEM((n // inner, part, breadth), BF16),
            strip,
            square,
            pltpu.SemaphoreType.DMA((11,)),
            pltpu.SemaphoreType.DMA((7, n)),
            pltpu.SemaphoreType.DMA((7, n)),
            pltpu.SemaphoreType.DMA((2, everyone)),
            pltpu.SemaphoreType.DMA((2, everyone)),
            pltpu.SemaphoreType.DMA((n // inner,)),
            pltpu.SemaphoreType.DMA((n // inner,)),
        ],
        compiler_params=pltpu.CompilerParams(
            collective_id=0, has_side_effects=True, vmem_limit_bytes=40 * 1024 * 1024
        ),
    )(
        *(
            pltpu.with_memory_space_constraint(value, pltpu.HBM)
            for value in (
                features,
                history,
                new_owner,
                pull_rows.reshape(n, 1, per_peer),
                occupancy,
                adj_local,
                adj_boundary,
                w_first,
                bias_first.reshape(1, breadth),
                w_second,
                cotangent,
            )
        )
    )
    return store(*results)


def near_width(n):
    return 2 if n % 2 == 0 else 1


def fits(peers, height, pulled, breadth, reps):
    return (
        height % (128 * peers) == 0
        and pulled == 128 * peers
        and breadth % (16 * near_width(peers) * reps) == 0
    )


def expand(occupied):
    return jnp.repeat(jnp.repeat(occupied, 128, axis=0), 128, axis=1).astype(jnp.bfloat16)


def dense_terms(owned, remote, adj_local, adj_boundary, occupancy):
    height = owned.shape[0]
    full_mask = expand(occupancy)
    local_tile = adj_local * full_mask[:, :height]
    edge_tile = adj_boundary * full_mask[:, height:]
    summed = jnp.dot(local_tile, owned, preferred_element_type=jnp.float32)
    summed = summed + jnp.dot(edge_tile, remote, preferred_element_type=jnp.float32)
    partial_value = lax.dot_general(
        edge_tile, owned, (((0,), (0,)), ((), ())), preferred_element_type=jnp.float32
    )
    return (summed, partial_value)


def body(
    features,
    history,
    new_owner,
    pull_rows,
    occupancy,
    adj_local,
    adj_boundary,
    w_first,
    bias_first,
    w_second,
    cotangent,
):
    peer_count = lax.axis_size("dev")
    height, breadth = features.shape
    cluster = height // peer_count
    pulled = pull_rows.shape[0]
    per_peer = pulled // peer_count
    everyone = peer_count * lax.axis_size("rep")
    if fits(peer_count, height, pulled, breadth, lax.axis_size("rep")):
        return fused(
            features,
            history,
            new_owner,
            pull_rows,
            occupancy,
            adj_local,
            adj_boundary,
            w_first,
            bias_first,
            w_second,
            cotangent,
        )
    indices = jnp.arange(peer_count, dtype=jnp.int32)
    matches = (new_owner[0][:, None] == indices[None, :]).astype(jnp.int32)
    inverse = jnp.sum(matches * indices[:, None], axis=0)

    def arrange(values):
        return values.reshape(peer_count, cluster, breadth)[inverse]

    requests = lax.all_to_all(
        pull_rows.reshape(peer_count, per_peer), "dev", split_axis=0, concat_axis=0, tiled=True
    ).reshape(pulled)

    def fetch_rows(values):
        return values[requests].reshape(peer_count, per_peer, breadth)

    selector = (requests[None, :] == jnp.arange(height, dtype=jnp.int32)[:, None]).astype(
        jnp.bfloat16
    )

    def collect(received):
        return jnp.dot(
            selector, received.reshape(pulled, breadth), preferred_element_type=jnp.float32
        )

    def layer_terms(owned, remote):
        return dense_terms(owned, remote, adj_local, adj_boundary, occupancy)

    moved_x, moved_h = (
        lax.all_to_all(arrange(features), "dev", split_axis=0, concat_axis=0, tiled=True),
        lax.all_to_all(arrange(history), "dev", split_axis=0, concat_axis=0, tiled=True),
    )
    own_x = moved_x.reshape(height, breadth)
    own_h = moved_h.reshape(height, breadth)
    far_x, far_h = (
        lax.all_to_all(fetch_rows(own_x), "dev", split_axis=0, concat_axis=0, tiled=True),
        lax.all_to_all(fetch_rows(own_h), "dev", split_axis=0, concat_axis=0, tiled=True),
    )
    summed_one, partial_one = layer_terms(own_x, far_x.reshape(pulled, breadth))
    pushed_one = lax.all_to_all(
        partial_one.astype(jnp.bfloat16).reshape(peer_count, per_peer, breadth),
        "dev",
        split_axis=0,
        concat_axis=0,
        tiled=True,
    )
    far_h = far_h.reshape(pulled, breadth)
    aggregate_one = (summed_one + collect(pushed_one)).astype(jnp.bfloat16)
    hidden = jnp.maximum(
        jnp.dot(aggregate_one, w_first, preferred_element_type=jnp.float32) + bias_first, 0.0
    ).astype(jnp.bfloat16)
    summed_two, partial_two = layer_terms(hidden, far_h)
    pushed_two = lax.all_to_all(
        partial_two.astype(jnp.bfloat16).reshape(peer_count, per_peer, breadth),
        "dev",
        split_axis=0,
        concat_axis=0,
        tiled=True,
    )
    aggregate_two = (summed_two + collect(pushed_two)).astype(jnp.bfloat16)
    output = jnp.dot(aggregate_two, w_second, preferred_element_type=jnp.float32).astype(
        jnp.bfloat16
    )
    local_grad = lax.dot_general(
        aggregate_two, cotangent, (((0,), (0,)), ((), ())), preferred_element_type=jnp.float32
    )
    slices = lax.all_to_all(
        local_grad.reshape(everyone, breadth // everyone, breadth),
        ("dev", "rep"),
        split_axis=0,
        concat_axis=0,
        tiled=True,
    )
    gradient = lax.all_gather(jnp.sum(slices, axis=0), ("dev", "rep"), axis=0, tiled=True)
    return (hidden, output, gradient)


def solution(mesh):
    return jax.shard_map(
        body,
        mesh=mesh,
        in_specs=(
            P(("dev", "rep"), None),
            P(("dev", "rep"), None),
            P(("dev", "rep"), None),
            P(("dev", "rep")),
            P(("dev", "rep"), None),
            P(("dev", "rep"), None),
            P(("dev", "rep"), None),
            P(),
            P(),
            P(),
            P(("dev", "rep"), None),
        ),
        out_specs=(P(("dev", "rep"), None), P(("dev", "rep"), None), P()),
        check_vma=False,
    )
```

```python
import functools

import jax
import jax.numpy as jnp
from jax import lax
from jax.experimental import pallas as pl
from jax.experimental.pallas import tpu as pltpu
from jax.sharding import PartitionSpec as P

MESH = pl.DeviceIdType.MESH
F32 = jnp.float32
BF16 = jnp.bfloat16
ASK, ASK_H, MOVE_X, FAR_X, H_ONE, H_TWO, PUSH_ONE, PUSH_TWO = range(8)


def step_kernel(
    n,
    reps,
    inner,
    features_hbm,
    history_hbm,
    new_owner_hbm,
    pulls_hbm,
    lists_hbm,
    occupancy_hbm,
    adj_local_hbm,
    adj_edge_hbm,
    w_first_hbm,
    bias_first_hbm,
    w_second_hbm,
    cotangent_hbm,
    hidden,
    output_out,
    grad_out,
    flag_out,
    features,
    history,
    new_owner,
    pulls,
    lists,
    occupancy,
    w_first,
    bias_first,
    w_second,
    local,
    edge,
    edge_t,
    cotangent,
    asked,
    codes,
    asked_h,
    pick,
    pick_t,
    pick_h,
    place,
    send_x,
    by_owner,
    own_x,
    send_far_x,
    send_rows,
    far_x,
    rows_in,
    far_h,
    send_one,
    send_two,
    push_one,
    push_two,
    acc,
    agg,
    grad_mine,
    grad_near,
    strip_mine,
    strip_far,
    total_mine,
    grad_all,
    flag_mine,
    flag_all,
    load_sem,
    send_sem,
    recv_sem,
    near_send,
    near_recv,
    far_send,
    far_recv,
    flag_send,
    flag_recv,
):
    me = lax.axis_index("dev")
    my_rep = lax.axis_index("rep")
    height, breadth = features.shape
    cluster = height // n
    per_peer = pulls.shape[2]
    pulled = n * per_peer
    tile = height // occupancy.shape[0]
    band = min(256, height)
    room = send_rows.shape[1]
    early = early_rows(room)
    wide = codes.shape[2] - per_peer

    def peer(off):
        return lax.rem(me + off, n)

    def rep_peer(off):
        return lax.rem(my_rep + off, reps)

    everyone = inner * reps
    outer = n // inner
    line = me // inner
    spot = lax.rem(me, inner) * reps + my_rep

    def near(off):
        return lax.rem(spot + off, everyone)

    def near_id(at):
        return {"dev": line * inner + at // reps, "rep": lax.rem(at, reps)}

    def far(off):
        return lax.rem(line + off, outer)

    def far_id(at):
        return {"dev": at * inner + lax.rem(me, inner)}

    barrier = pltpu.get_barrier_semaphore()
    for off in range(1, n):
        pl.semaphore_signal(barrier, inc=1, device_id={"dev": peer(off)}, device_id_type=MESH)
    for side in range(inner):
        for off in range(1, reps):
            pl.semaphore_signal(
                barrier,
                inc=1,
                device_id={
                    "dev": line * inner + lax.rem(me + side, inner),
                    "rep": rep_peer(off),
                },
                device_id_type=MESH,
            )

    loads = [
        pltpu.make_async_copy(source, target, load_sem.at[i])
        for i, (source, target) in enumerate(
            (
                (new_owner_hbm, new_owner),
                (features_hbm, features),
                (lists_hbm, lists),
                (pulls_hbm, pulls),
                (history_hbm, history),
                (occupancy_hbm, occupancy),
                (adj_edge_hbm, edge),
                (adj_local_hbm, local),
                (w_first_hbm, w_first),
                (bias_first_hbm, bias_first),
                (w_second_hbm, w_second),
                (cotangent_hbm, cotangent),
            )
        )
    ]
    for load in loads:
        load.start()

    def cluster_for(source, owner):
        block = jnp.zeros((cluster, breadth), BF16)
        for j in range(n):
            chosen = jnp.where(new_owner[0, j] == owner, 1.0, 0.0)
            weight = jnp.full((cluster, breadth), chosen, F32).astype(BF16)
            block = block + source[j * cluster : (j + 1) * cluster, :] * weight
        return block

    def outgoing(phase, src, dst, to, slot):
        return pltpu.make_async_remote_copy(
            src_ref=src.at[to],
            dst_ref=dst.at[slot],
            send_sem=send_sem.at[phase, to],
            recv_sem=recv_sem.at[phase, slot],
            device_id={"dev": to},
            device_id_type=MESH,
        )

    def send(phase, src, dst, off):
        outgoing(phase, src, dst, peer(off), me).start()

    def receive(phase, src, dst):
        for off in range(1, n):
            other = peer(off)
            outgoing(phase, src, dst, other, other).wait_recv()

    def finish(phase, src, dst):
        for off in range(1, n):
            outgoing(phase, src, dst, peer(off), me).wait_send()

    def slots():
        upper = jnp.where(
            lax.broadcasted_iota(jnp.int32, (per_peer, per_peer), 0)
            <= lax.broadcasted_iota(jnp.int32, (per_peer, per_peer), 1),
            1.0,
            0.0,
        ).astype(BF16)
        origin = lax.broadcasted_iota(jnp.int32, (n, per_peer), 0)
        seats = lax.broadcasted_iota(jnp.int32, (wide, per_peer), 0).astype(F32)
        held, within = [], []
        for e in range(n):
            row = jnp.broadcast_to(lists[e : e + 1, :], (n, per_peer)) - origin * cluster
            held.append(jnp.where((row >= 0) & (row < cluster), 1.0, 0.0))
            within.append(row.astype(F32))
        stacked = jnp.concatenate(held, axis=0).astype(BF16)
        prefix = jnp.dot(stacked, upper, preferred_element_type=F32)
        totals = jnp.dot(
            stacked, jnp.ones((per_peer, per_peer), BF16), preferred_element_type=F32
        )
        before = jnp.full((n, per_peer), -1.0, F32)
        over = jnp.zeros((n, per_peer), F32)
        table = jnp.zeros((2 * n, wide), F32)
        places = []
        for e in range(n):
            seat = held[e] * (prefix[e * n : (e + 1) * n, :] + before)
            before = before + totals[e * n : (e + 1) * n, :]
            over = jnp.maximum(over, seat)
            places.append(
                jnp.sum(seat + held[e] * (origin * room).astype(F32), axis=0, keepdims=True)
            )
            mine = jnp.sum(seat, axis=0, keepdims=True)
            taken = jnp.where(seats == mine, 1.0, 0.0).astype(BF16)
            entry = jnp.concatenate([held[e] * float(e), held[e] * within[e]], axis=0)
            table = table + lax.dot_general(
                entry.astype(BF16), taken, (((1,), (1,)), ((), ())), preferred_element_type=F32
            )
        found = (table[:n, :] * float(cluster) + table[n:, :]).astype(jnp.int32)
        full = jnp.where(jnp.max(over, axis=0, keepdims=True) >= float(room), 1, 0)
        for d in range(n):
            codes[d, :, :wide] = found[d : d + 1, :]
            codes[d, :, wide:] = full
        return places

    loads[2].wait()
    places = slots()
    loads[0].wait()
    loads[1].wait()
    for off in range(1, n):
        send_x[peer(off)] = cluster_for(features, peer(off))
    own_x[me] = cluster_for(features, me)
    loads[3].wait()
    pl.semaphore_wait(barrier, n - 1 + inner * (reps - 1))
    for off in range(1, n):
        send(ASK_H, codes, asked_h, off)
    for off in range(1, n):
        send(ASK, pulls, asked, off)
    for off in range(1, n):
        send(MOVE_X, send_x, own_x, off)
    asked[me] = pulls[me]
    asked_h[me] = codes[me]
    loads[4].wait()
    for e in range(n):
        by_owner[e] = cluster_for(history, e)
    for e in range(n):
        turned = jnp.broadcast_to(places[e], (per_peer, per_peer)).T
        for c in range(n * room // per_peer):
            lanes = lax.broadcasted_iota(jnp.int32, (per_peer, per_peer), 1) + c * per_peer
            place[e * per_peer : (e + 1) * per_peer, c * per_peer : (c + 1) * per_peer] = (
                jnp.where(turned == lanes.astype(F32), 1.0, 0.0).astype(BF16)
            )

    def flag_copy(to, slot):
        return pltpu.make_async_remote_copy(
            src_ref=flag_mine,
            dst_ref=flag_all.at[slot],
            send_sem=flag_send.at[to],
            recv_sem=flag_recv.at[slot],
            device_id={"rep": to},
            device_id_type=MESH,
        )

    receive(ASK_H, codes, asked_h)
    full = asked_h[0, :, wide:]
    for d in range(1, n):
        full = jnp.maximum(full, asked_h[d, :, wide:])
    flag_mine[...] = full
    for off in range(1, reps):
        flag_copy(rep_peer(off), my_rep).start()
    flag_all[my_rep] = full
    for d in range(n):
        for top in range(0, room, per_peer):
            size = min(per_peer, room - top)
            turned = jnp.broadcast_to(asked_h[d, :, top : top + per_peer], (per_peer, per_peer)).T
            for c in range(height // per_peer):
                lanes = lax.broadcasted_iota(jnp.int32, (size, per_peer), 1) + c * per_peer
                pick_h[
                    d * room + top : d * room + top + size, c * per_peer : (c + 1) * per_peer
                ] = jnp.where(turned[:size, :] == lanes, 1.0, 0.0).astype(BF16)

    def rows_copy(phase, start, size, to, slot):
        return pltpu.make_async_remote_copy(
            src_ref=send_rows.at[to, pl.ds(start, size)],
            dst_ref=rows_in.at[slot, pl.ds(start, size)],
            send_sem=send_sem.at[phase, to],
            recv_sem=recv_sem.at[phase, slot],
            device_id={"dev": to},
            device_id_type=MESH,
        )

    def rows_for(to):
        rows = pl.ds(pl.multiple_of(to * room, 16), room)
        values = by_owner[...].reshape(n * cluster, breadth)
        return jnp.dot(pick_h[rows, :], values, preferred_element_type=F32).astype(BF16)

    def rows_out(off, carry):
        send_rows[peer(off)] = rows_for(peer(off))
        rows_copy(H_ONE, 0, early, peer(off), me).start()
        return carry

    lax.fori_loop(1, n, rows_out, 0)
    rows_in[me] = rows_for(me)

    loads[5].wait()
    loads[6].wait()
    for i in range(height // tile):
        for j in range(pulled // tile):
            kept = occupancy[i, height // tile + j].astype(F32)
            rows, cols = pl.ds(i * tile, tile), pl.ds(j * tile, tile)
            part = (edge[rows, cols].astype(F32) * kept).astype(BF16)
            edge[rows, cols] = part
            edge_t[cols, rows] = part.T
    loads[7].wait()
    for i in range(height // tile):
        for j in range(height // tile):
            kept = occupancy[i, j].astype(F32)
            rows, cols = pl.ds(i * tile, tile), pl.ds(j * tile, tile)
            local[rows, cols] = (local[rows, cols].astype(F32) * kept).astype(BF16)

    receive(ASK, pulls, asked)
    for d in range(n):
        wanted = asked[d]
        rows = lax.broadcasted_iota(jnp.int32, (height, per_peer), 0)
        pick[:, d * per_peer : (d + 1) * per_peer] = jnp.where(rows == wanted, 1.0, 0.0).astype(
            BF16
        )
        turned = jnp.broadcast_to(wanted, (per_peer, per_peer)).T
        lanes = lax.broadcasted_iota(jnp.int32, (per_peer, per_peer), 1)
        for c in range(height // per_peer):
            pick_t[d * per_peer : (d + 1) * per_peer, c * per_peer : (c + 1) * per_peer] = (
                jnp.where(turned == lanes + c * per_peer, 1.0, 0.0).astype(BF16)
            )

    def blocks_out(phase, left, right, src, dst):
        values = right[...].reshape(left.shape[1], breadth)

        def block(to):
            rows = pl.ds(pl.multiple_of(to * per_peer, per_peer), per_peer)
            return jnp.dot(left[rows, :], values, preferred_element_type=F32).astype(BF16)

        def one(off, carry):
            src[peer(off)] = block(peer(off))
            send(phase, src, dst, off)
            return carry

        lax.fori_loop(1, n, one, 0)
        dst[me] = block(me)

    def bands(body):
        def one(i, carry):
            body(pl.ds(pl.multiple_of(i * band, band), band))
            return carry

        lax.fori_loop(0, height // band, one, 0)

    def times(left, rows, right):
        values = right[...].reshape(left.shape[1], breadth)
        return jnp.dot(left[rows, :], values, preferred_element_type=F32)

    receive(MOVE_X, send_x, own_x)
    blocks_out(FAR_X, pick_t, own_x, send_far_x, far_x)
    blocks_out(PUSH_ONE, edge_t, own_x, send_one, push_one)
    for off in range(1, n):
        rows_copy(H_TWO, early, room - early, peer(off), me).start()

    def local_one(rows):
        acc[rows, :] = times(local, rows, own_x)

    bands(local_one)
    receive(FAR_X, send_far_x, far_x)

    def edge_one(rows):
        acc[rows, :] = acc[rows, :] + times(edge, rows, far_x)

    bands(edge_one)
    receive(PUSH_ONE, send_one, push_one)

    def first(rows):
        total = (acc[rows, :] + times(pick, rows, push_one)).astype(BF16)
        value = jnp.dot(total, w_first[...], preferred_element_type=F32) + bias_first[...]
        value = jnp.maximum(value, 0.0).astype(BF16)
        hidden[rows, :] = value

    loads[8].wait()
    loads[9].wait()
    bands(first)
    blocks_out(PUSH_TWO, edge_t, hidden, send_two, push_two)

    def local_two(rows):
        acc[rows, :] = times(local, rows, hidden)

    bands(local_two)
    for off in range(1, n):
        rows_copy(H_ONE, 0, early, peer(off), peer(off)).wait_recv()
    for off in range(1, n):
        rows_copy(H_TWO, early, room - early, peer(off), peer(off)).wait_recv()

    def gather_h(rows):
        far_h[rows, :] = times(place, rows, rows_in).astype(BF16)

    bands(gather_h)

    def edge_two(rows):
        acc[rows, :] = acc[rows, :] + times(edge, rows, far_h)

    bands(edge_two)
    loads[10].wait()
    loads[11].wait()
    for off in range(1, reps):
        flag_copy(rep_peer(off), rep_peer(off)).wait_recv()
    full = flag_all[0]
    for r in range(1, reps):
        full = jnp.maximum(full, flag_all[r])
    flag_out[0] = jnp.where(jnp.max(full.astype(F32)) > 0.5, 1, 0)
    receive(PUSH_TWO, send_two, push_two)

    def second(rows):
        agg[rows, :] = (acc[rows, :] + times(pick, rows, push_two)).astype(BF16)

    bands(second)
    grad = lax.dot_general(
        agg[...], cotangent[...], (((0,), (0,)), ((), ())), preferred_element_type=F32
    )
    grad_mine[...] = grad.reshape(grad_mine.shape).astype(BF16)

    def near_copy(phase, src, dst, to, slot):
        return pltpu.make_async_remote_copy(
            src_ref=src,
            dst_ref=dst.at[slot],
            send_sem=near_send.at[phase, to],
            recv_sem=near_recv.at[phase, slot],
            device_id=near_id(to),
            device_id_type=MESH,
        )

    def far_copy(to, slot):
        return pltpu.make_async_remote_copy(
            src_ref=strip_mine,
            dst_ref=strip_far.at[slot],
            send_sem=far_send.at[to],
            recv_sem=far_recv.at[slot],
            device_id=far_id(to),
            device_id_type=MESH,
        )

    for off in range(1, everyone):
        near_copy(0, grad_mine.at[near(off)], grad_near, near(off), spot).start()

    def last(rows):
        output_out[rows, :] = jnp.dot(
            agg[rows, :], w_second[...], preferred_element_type=F32
        ).astype(BF16)

    bands(last)
    total = grad_mine[spot].astype(F32)
    for off in range(1, everyone):
        near_copy(0, grad_mine.at[near(off)], grad_near, near(off), near(off)).wait_recv()
        total = total + grad_near[near(off)].astype(F32)
    strip_mine[...] = total.astype(BF16)
    for off in range(1, outer):
        far_copy(far(off), line).start()
    strip_far[line] = strip_mine[...]
    for off in range(1, outer):
        far_copy(far(off), far(off)).wait_recv()
    total = strip_far[0].astype(F32)
    for z in range(1, outer):
        total = total + strip_far[z].astype(F32)
    total_mine[...] = total.astype(BF16)
    for off in range(1, everyone):
        near_copy(1, total_mine, grad_all, near(off), spot).start()
    grad_all[spot] = total_mine[...]
    for off in range(1, everyone):
        near_copy(1, total_mine, grad_all, near(off), near(off)).wait_recv()
    grad_out[...] = grad_all[...].astype(F32).reshape(grad_out.shape)

    finish(ASK, pulls, asked)
    finish(MOVE_X, send_x, own_x)
    finish(FAR_X, send_far_x, far_x)
    finish(ASK_H, codes, asked_h)
    for off in range(1, n):
        rows_copy(H_ONE, 0, early, peer(off), me).wait_send()
        rows_copy(H_TWO, early, room - early, peer(off), me).wait_send()
    for off in range(1, reps):
        flag_copy(rep_peer(off), my_rep).wait_send()
    finish(PUSH_ONE, send_one, push_one)
    finish(PUSH_TWO, send_two, push_two)
    for off in range(1, everyone):
        near_copy(0, grad_mine.at[near(off)], grad_near, near(off), spot).wait_send()
        near_copy(1, total_mine, grad_all, near(off), spot).wait_send()
    for off in range(1, outer):
        far_copy(far(off), line).wait_send()


def store_kernel(count, *refs):
    sems = refs[-1]
    copies = [
        pltpu.make_async_copy(refs[i], refs[count + i], sems.at[i]) for i in range(count)
    ]
    for copy in copies:
        copy.start()
    for copy in copies:
        copy.wait()


def store(*values):
    count = len(values)
    return pl.pallas_call(
        functools.partial(store_kernel, count),
        out_shape=tuple(pltpu.HBM(v.shape, v.dtype) for v in values),
        in_specs=[pl.BlockSpec(memory_space=pltpu.VMEM)] * count,
        out_specs=tuple(pl.BlockSpec(memory_space=pl.ANY) for _ in values),
        scratch_shapes=[pltpu.SemaphoreType.DMA((count,))],
        compiler_params=pltpu.CompilerParams(vmem_limit_bytes=8 * 1024 * 1024),
    )(*values)


def fused(
    features,
    history,
    new_owner,
    pull_rows,
    occupancy,
    adj_local,
    adj_boundary,
    w_first,
    bias_first,
    w_second,
    cotangent,
):
    n, reps = lax.axis_size("dev"), lax.axis_size("rep")
    height, breadth = features.shape
    cluster = height // n
    pulled = pull_rows.shape[0]
    per_peer = pulled // n
    inner = near_width(n)
    everyone = inner * reps
    part = breadth // everyone
    vmem = pl.BlockSpec(memory_space=pltpu.VMEM)
    anywhere = pl.BlockSpec(memory_space=pltpu.HBM)
    moved = pltpu.VMEM((n, cluster, breadth), BF16)
    listed = pltpu.VMEM((n, per_peer, breadth), BF16)
    square = pltpu.VMEM((everyone, part, breadth), BF16)
    strip = pltpu.VMEM((part, breadth), BF16)
    weight = pltpu.VMEM((breadth, breadth), BF16)
    nodes = pltpu.VMEM((height, breadth), BF16)
    room = row_room(per_peer)
    wide = -(-room // 128) * 128
    asks = pltpu.VMEM((n, 1, wide + per_peer), jnp.int32)
    rows = pltpu.VMEM((n, room, breadth), BF16)
    results = pl.pallas_call(
        functools.partial(step_kernel, n, reps, inner),
        out_shape=(
            pltpu.VMEM((height, breadth), BF16),
            pltpu.VMEM((height, breadth), BF16),
            pltpu.VMEM((breadth, breadth), F32),
            pltpu.SMEM((1,), jnp.int32),
        ),
        in_specs=[anywhere] * 12,
        out_specs=(vmem, vmem, vmem, pl.BlockSpec(memory_space=pltpu.SMEM)),
        scratch_shapes=[
            nodes,
            nodes,
            pltpu.SMEM(new_owner.shape, jnp.int32),
            pltpu.VMEM((n, 1, per_peer), jnp.int32),
            pltpu.VMEM((n, per_peer), jnp.int32),
            pltpu.SMEM(occupancy.shape, jnp.int32),
            weight,
            pltpu.VMEM((1, breadth), F32),
            weight,
            pltpu.VMEM((height, height), BF16),
            pltpu.VMEM((height, pulled), BF16),
            pltpu.VMEM((pulled, height), BF16),
            nodes,
            pltpu.VMEM((n, 1, per_peer), jnp.int32),
            asks,
            asks,
            pltpu.VMEM((height, pulled), BF16),
            pltpu.VMEM((pulled, height), BF16),
            pltpu.VMEM((n * room, height), BF16),
            pltpu.VMEM((pulled, n * room), BF16),
            moved,
            moved,
            moved,
            listed,
            rows,
            listed,
            rows,
            pltpu.VMEM((pulled, breadth), BF16),
            listed,
            listed,
            listed,
            listed,
            pltpu.VMEM((height, breadth), F32),
            nodes,
            square,
            square,
            strip,
            pltpu.VMEM((n // inner, part, breadth), BF16),
            strip,
            square,
            pltpu.VMEM((1, per_peer), jnp.int32),
            pltpu.VMEM((reps, 1, per_peer), jnp.int32),
            pltpu.SemaphoreType.DMA((12,)),
            pltpu.SemaphoreType.DMA((8, n)),
            pltpu.SemaphoreType.DMA((8, n)),
            pltpu.SemaphoreType.DMA((2, everyone)),
            pltpu.SemaphoreType.DMA((2, everyone)),
            pltpu.SemaphoreType.DMA((n // inner,)),
            pltpu.SemaphoreType.DMA((n // inner,)),
            pltpu.SemaphoreType.DMA((reps,)),
            pltpu.SemaphoreType.DMA((reps,)),
        ],
        compiler_params=pltpu.CompilerParams(
            collective_id=0, has_side_effects=True, vmem_limit_bytes=40 * 1024 * 1024
        ),
    )(
        *(
            pltpu.with_memory_space_constraint(value, pltpu.HBM)
            for value in (
                features,
                history,
                new_owner,
                pull_rows.reshape(n, 1, per_peer),
                pull_rows.reshape(n, per_peer),
                occupancy,
                adj_local,
                adj_boundary,
                w_first,
                bias_first.reshape(1, breadth),
                w_second,
                cotangent,
            )
        )
    )
    return results


def row_room(per_peer):
    return per_peer * 11 // 8


def early_rows(room):
    return room // 32 * 16


def near_width(n):
    return 2 if n % 2 == 0 else 1


def fits(peers, height, pulled, breadth, reps):
    return (
        height % (128 * peers) == 0
        and pulled == 128 * peers
        and peers * row_room(128) % 128 == 0
        and breadth % (16 * near_width(peers) * reps) == 0
    )


def expand(occupied):
    return jnp.repeat(jnp.repeat(occupied, 128, axis=0), 128, axis=1).astype(jnp.bfloat16)


def dense_terms(owned, remote, adj_local, adj_boundary, occupancy):
    height = owned.shape[0]
    full_mask = expand(occupancy)
    local_tile = adj_local * full_mask[:, :height]
    edge_tile = adj_boundary * full_mask[:, height:]
    summed = jnp.dot(local_tile, owned, preferred_element_type=jnp.float32)
    summed = summed + jnp.dot(edge_tile, remote, preferred_element_type=jnp.float32)
    partial_value = lax.dot_general(
        edge_tile, owned, (((0,), (0,)), ((), ())), preferred_element_type=jnp.float32
    )
    return (summed, partial_value)


def body(*args):
    features, pull_rows = args[0], args[3]
    peer_count = lax.axis_size("dev")
    height, breadth = features.shape
    if not fits(peer_count, height, pull_rows.shape[0], breadth, lax.axis_size("rep")):
        return plain(*args)
    *results, full = fused(*args)
    return lax.cond(full[0] > 0, lambda: store(*plain(*args)), lambda: store(*results))


def plain(
    features,
    history,
    new_owner,
    pull_rows,
    occupancy,
    adj_local,
    adj_boundary,
    w_first,
    bias_first,
    w_second,
    cotangent,
):
    peer_count = lax.axis_size("dev")
    height, breadth = features.shape
    cluster = height // peer_count
    pulled = pull_rows.shape[0]
    per_peer = pulled // peer_count
    everyone = peer_count * lax.axis_size("rep")
    indices = jnp.arange(peer_count, dtype=jnp.int32)
    matches = (new_owner[0][:, None] == indices[None, :]).astype(jnp.int32)
    inverse = jnp.sum(matches * indices[:, None], axis=0)

    def arrange(values):
        return values.reshape(peer_count, cluster, breadth)[inverse]

    requests = lax.all_to_all(
        pull_rows.reshape(peer_count, per_peer), "dev", split_axis=0, concat_axis=0, tiled=True
    ).reshape(pulled)

    def fetch_rows(values):
        return values[requests].reshape(peer_count, per_peer, breadth)

    selector = (requests[None, :] == jnp.arange(height, dtype=jnp.int32)[:, None]).astype(
        jnp.bfloat16
    )

    def collect(received):
        return jnp.dot(
            selector, received.reshape(pulled, breadth), preferred_element_type=jnp.float32
        )

    def layer_terms(owned, remote):
        return dense_terms(owned, remote, adj_local, adj_boundary, occupancy)

    moved_x, moved_h = (
        lax.all_to_all(arrange(features), "dev", split_axis=0, concat_axis=0, tiled=True),
        lax.all_to_all(arrange(history), "dev", split_axis=0, concat_axis=0, tiled=True),
    )
    own_x = moved_x.reshape(height, breadth)
    own_h = moved_h.reshape(height, breadth)
    far_x, far_h = (
        lax.all_to_all(fetch_rows(own_x), "dev", split_axis=0, concat_axis=0, tiled=True),
        lax.all_to_all(fetch_rows(own_h), "dev", split_axis=0, concat_axis=0, tiled=True),
    )
    summed_one, partial_one = layer_terms(own_x, far_x.reshape(pulled, breadth))
    pushed_one = lax.all_to_all(
        partial_one.astype(jnp.bfloat16).reshape(peer_count, per_peer, breadth),
        "dev",
        split_axis=0,
        concat_axis=0,
        tiled=True,
    )
    far_h = far_h.reshape(pulled, breadth)
    aggregate_one = (summed_one + collect(pushed_one)).astype(jnp.bfloat16)
    hidden = jnp.maximum(
        jnp.dot(aggregate_one, w_first, preferred_element_type=jnp.float32) + bias_first, 0.0
    ).astype(jnp.bfloat16)
    summed_two, partial_two = layer_terms(hidden, far_h)
    pushed_two = lax.all_to_all(
        partial_two.astype(jnp.bfloat16).reshape(peer_count, per_peer, breadth),
        "dev",
        split_axis=0,
        concat_axis=0,
        tiled=True,
    )
    aggregate_two = (summed_two + collect(pushed_two)).astype(jnp.bfloat16)
    output = jnp.dot(aggregate_two, w_second, preferred_element_type=jnp.float32).astype(
        jnp.bfloat16
    )
    local_grad = lax.dot_general(
        aggregate_two, cotangent, (((0,), (0,)), ((), ())), preferred_element_type=jnp.float32
    )
    slices = lax.all_to_all(
        local_grad.reshape(everyone, breadth // everyone, breadth),
        ("dev", "rep"),
        split_axis=0,
        concat_axis=0,
        tiled=True,
    )
    gradient = lax.all_gather(jnp.sum(slices, axis=0), ("dev", "rep"), axis=0, tiled=True)
    return (hidden, output, gradient)


def solution(mesh):
    return jax.shard_map(
        body,
        mesh=mesh,
        in_specs=(
            P(("dev", "rep"), None),
            P(("dev", "rep"), None),
            P(("dev", "rep"), None),
            P(("dev", "rep")),
            P(("dev", "rep"), None),
            P(("dev", "rep"), None),
            P(("dev", "rep"), None),
            P(),
            P(),
            P(),
            P(("dev", "rep"), None),
        ),
        out_specs=(P(("dev", "rep"), None), P(("dev", "rep"), None), P()),
        check_vma=False,
    )
```

```python
import functools

import jax
import jax.numpy as jnp
from jax import lax
from jax.experimental import pallas as pl
from jax.experimental.pallas import tpu as pltpu
from jax.sharding import PartitionSpec as P

MESH = pl.DeviceIdType.MESH
F32 = jnp.float32
BF16 = jnp.bfloat16
ASK, ASK_H, MOVE_X, FAR_X, H_ONE, H_TWO, NEAR_X, PUSH_ONE, PUSH_TWO = range(9)


def step_kernel(
    n,
    reps,
    inner,
    features_hbm,
    history_hbm,
    new_owner_hbm,
    pulls_hbm,
    lists_hbm,
    occupancy_hbm,
    adj_local_hbm,
    adj_edge_hbm,
    w_first_hbm,
    bias_first_hbm,
    w_second_hbm,
    cotangent_hbm,
    hidden,
    output_out,
    grad_out,
    flag_out,
    features,
    history,
    new_owner,
    pulls,
    lists,
    occupancy,
    w_first,
    bias_first,
    w_second,
    local,
    edge,
    edge_t,
    cotangent,
    asked,
    codes,
    asked_h,
    pick,
    pick_t,
    pick_h,
    place,
    pick_n,
    place_x,
    seat_x,
    send_x,
    by_owner,
    own_x,
    send_far_x,
    send_rows,
    send_near,
    far_x,
    mix,
    rows_in,
    far_h,
    send_one,
    send_two,
    push_one,
    push_two,
    acc,
    agg,
    grad_mine,
    grad_near,
    strip_mine,
    strip_far,
    total_mine,
    grad_all,
    flag_mine,
    flag_all,
    load_sem,
    send_sem,
    recv_sem,
    near_send,
    near_recv,
    far_send,
    far_recv,
    flag_send,
    flag_recv,
):
    me = lax.axis_index("dev")
    my_rep = lax.axis_index("rep")
    height, breadth = features.shape
    cluster = height // n
    per_peer = pulls.shape[2]
    pulled = n * per_peer
    tile = height // occupancy.shape[0]
    band = min(256, height)
    room = send_rows.shape[1]
    early = early_rows(room)
    wide = codes.shape[2] - 3 * per_peer
    half = n // 2
    depth = mix.shape[1]
    cross = cross_rows(per_peer)
    home = lax.rem(me, half)
    side = me // half

    def beside(off):
        return side * half + lax.rem(home + off, half)

    def across(off):
        return (1 - side) * half + lax.rem(home + off, half)

    def peer(off):
        return lax.rem(me + off, n)

    def rep_peer(off):
        return lax.rem(my_rep + off, reps)

    everyone = inner * reps
    outer = n // inner
    line = me // inner
    spot = lax.rem(me, inner) * reps + my_rep

    def near(off):
        return lax.rem(spot + off, everyone)

    def near_id(at):
        return {"dev": line * inner + at // reps, "rep": lax.rem(at, reps)}

    def far(off):
        return lax.rem(line + off, outer)

    def far_id(at):
        return {"dev": at * inner + lax.rem(me, inner)}

    barrier = pltpu.get_barrier_semaphore()
    for off in range(1, n):
        pl.semaphore_signal(barrier, inc=1, device_id={"dev": peer(off)}, device_id_type=MESH)
    for lane in range(inner):
        for off in range(1, reps):
            pl.semaphore_signal(
                barrier,
                inc=1,
                device_id={
                    "dev": line * inner + lax.rem(me + lane, inner),
                    "rep": rep_peer(off),
                },
                device_id_type=MESH,
            )

    loads = [
        pltpu.make_async_copy(source, target, load_sem.at[i])
        for i, (source, target) in enumerate(
            (
                (new_owner_hbm, new_owner),
                (features_hbm, features),
                (lists_hbm, lists),
                (pulls_hbm, pulls),
                (history_hbm, history),
                (occupancy_hbm, occupancy),
                (adj_edge_hbm, edge),
                (adj_local_hbm, local),
                (w_first_hbm, w_first),
                (bias_first_hbm, bias_first),
                (w_second_hbm, w_second),
                (cotangent_hbm, cotangent),
            )
        )
    ]
    for load in loads:
        load.start()

    def cluster_for(source, owner):
        block = jnp.zeros((cluster, breadth), BF16)
        for j in range(n):
            chosen = jnp.where(new_owner[0, j] == owner, 1.0, 0.0)
            weight = jnp.full((cluster, breadth), chosen, F32).astype(BF16)
            block = block + source[j * cluster : (j + 1) * cluster, :] * weight
        return block

    def outgoing(phase, src, dst, to, slot):
        return pltpu.make_async_remote_copy(
            src_ref=src.at[to],
            dst_ref=dst.at[slot],
            send_sem=send_sem.at[phase, to],
            recv_sem=recv_sem.at[phase, slot],
            device_id={"dev": to},
            device_id_type=MESH,
        )

    def send(phase, src, dst, off):
        outgoing(phase, src, dst, peer(off), me).start()

    def receive(phase, src, dst):
        for off in range(1, n):
            other = peer(off)
            outgoing(phase, src, dst, other, other).wait_recv()

    def finish(phase, src, dst):
        for off in range(1, n):
            outgoing(phase, src, dst, peer(off), me).wait_send()

    def slots():
        upper = jnp.where(
            lax.broadcasted_iota(jnp.int32, (per_peer, per_peer), 0)
            <= lax.broadcasted_iota(jnp.int32, (per_peer, per_peer), 1),
            1.0,
            0.0,
        ).astype(BF16)
        origin = lax.broadcasted_iota(jnp.int32, (n, per_peer), 0)
        seats = lax.broadcasted_iota(jnp.int32, (wide, per_peer), 0).astype(F32)
        held, within = [], []
        for e in range(n):
            row = jnp.broadcast_to(lists[e : e + 1, :], (n, per_peer)) - origin * cluster
            held.append(jnp.where((row >= 0) & (row < cluster), 1.0, 0.0))
            within.append(row.astype(F32))
        stacked = jnp.concatenate(held, axis=0).astype(BF16)
        prefix = jnp.dot(stacked, upper, preferred_element_type=F32)
        totals = jnp.dot(
            stacked, jnp.ones((per_peer, per_peer), BF16), preferred_element_type=F32
        )
        before = jnp.full((n, per_peer), -1.0, F32)
        over = jnp.zeros((n, per_peer), F32)
        table = jnp.zeros((2 * n, wide), F32)
        lanes = seats[:per_peer]
        away = (origin // half != side).astype(F32)
        nearby = 1.0 - away
        spot_s = lax.rem(origin, half) + half
        behind = jnp.full((n, per_peer), -1.0, F32)
        table_n = jnp.zeros((2 * n, per_peer), F32)
        places = []
        for e in range(n):
            remote = jnp.where(e // half != side, 1.0, 0.0)
            ahead = prefix[e * n : (e + 1) * n, :]
            rank = jnp.sum(ahead * away, axis=0, keepdims=True) - 1.0
            gone = held[e] * away
            stays = held[e] * nearby * remote
            seat = stays * (ahead + behind)
            behind = behind + remote * totals[e * n : (e + 1) * n, :]
            over = jnp.maximum(over, seat + float(room - depth))
            over = jnp.maximum(over, remote * gone * rank + float(room - cross))
            seat_x[e] = jnp.sum(
                seat
                + stays * (spot_s * depth).astype(F32)
                + gone * (rank + float(e % half * depth)),
                axis=0,
                keepdims=True,
            )
            taken = jnp.where(lanes == rank, 1.0, 0.0).astype(BF16)
            entry = jnp.concatenate([gone * origin.astype(F32), gone * within[e]], axis=0)
            listed = lax.dot_general(
                entry.astype(BF16), taken, (((1,), (1,)), ((), ())), preferred_element_type=F32
            )
            listed = jnp.sum(
                listed[:n, :] * float(cluster) + listed[n:, :], axis=0, keepdims=True
            ).astype(jnp.int32)
            codes[e, :, wide + per_peer : wide + 2 * per_peer] = jnp.where(
                e // half != side, listed, lists[e : e + 1, :]
            )
            mine = jnp.sum(seat, axis=0, keepdims=True)
            taken = jnp.where(lanes == mine, 1.0, 0.0).astype(BF16)
            entry = jnp.concatenate([stays * float(e), stays * within[e]], axis=0)
            table_n = table_n + lax.dot_general(
                entry.astype(BF16), taken, (((1,), (1,)), ((), ())), preferred_element_type=F32
            )
        for e in range(n):
            seat = held[e] * (prefix[e * n : (e + 1) * n, :] + before)
            before = before + totals[e * n : (e + 1) * n, :]
            over = jnp.maximum(over, seat)
            places.append(
                jnp.sum(seat + held[e] * (origin * room).astype(F32), axis=0, keepdims=True)
            )
            mine = jnp.sum(seat, axis=0, keepdims=True)
            taken = jnp.where(seats == mine, 1.0, 0.0).astype(BF16)
            entry = jnp.concatenate([held[e] * float(e), held[e] * within[e]], axis=0)
            table = table + lax.dot_general(
                entry.astype(BF16), taken, (((1,), (1,)), ((), ())), preferred_element_type=F32
            )
        found = (table[:n, :] * float(cluster) + table[n:, :]).astype(jnp.int32)
        full = jnp.where(jnp.max(over, axis=0, keepdims=True) >= float(room), 1, 0)
        found_n = (table_n[:n, :] * float(cluster) + table_n[n:, :]).astype(jnp.int32)
        for d in range(n):
            codes[d, :, :wide] = found[d : d + 1, :]
            codes[d, :, wide : wide + per_peer] = full
            codes[d, :, wide + 2 * per_peer :] = found_n[d : d + 1, :]
        return places

    loads[2].wait()
    places = slots()
    loads[0].wait()
    loads[1].wait()
    for off in range(1, n):
        send_x[peer(off)] = cluster_for(features, peer(off))
    own_x[me] = cluster_for(features, me)
    send_x[me] = own_x[me]
    loads[3].wait()
    pl.semaphore_wait(barrier, n - 1 + inner * (reps - 1))
    for off in range(1, n):
        send(ASK_H, codes, asked_h, off)
    for off in range(1, n):
        send(ASK, pulls, asked, off)
    for off in range(1, n):
        send(MOVE_X, send_x, own_x, off)
    asked[me] = pulls[me]
    asked_h[me] = codes[me]
    loads[4].wait()
    for e in range(n):
        by_owner[e] = cluster_for(history, e)
    for e in range(n):
        turned = jnp.broadcast_to(places[e], (per_peer, per_peer)).T
        for c in range(n * room // per_peer):
            lanes = lax.broadcasted_iota(jnp.int32, (per_peer, per_peer), 1) + c * per_peer
            place[e * per_peer : (e + 1) * per_peer, c * per_peer : (c + 1) * per_peer] = (
                jnp.where(turned == lanes.astype(F32), 1.0, 0.0).astype(BF16)
            )

    def flag_copy(to, slot):
        return pltpu.make_async_remote_copy(
            src_ref=flag_mine,
            dst_ref=flag_all.at[slot],
            send_sem=flag_send.at[to],
            recv_sem=flag_recv.at[slot],
            device_id={"rep": to},
            device_id_type=MESH,
        )

    receive(ASK_H, codes, asked_h)
    full = asked_h[0, :, wide : wide + per_peer]
    for d in range(1, n):
        full = jnp.maximum(full, asked_h[d, :, wide : wide + per_peer])
    flag_mine[...] = full
    for off in range(1, reps):
        flag_copy(rep_peer(off), my_rep).start()
    flag_all[my_rep] = full
    for d in range(n):
        for top in range(0, room, per_peer):
            size = min(per_peer, room - top)
            turned = jnp.broadcast_to(asked_h[d, :, top : top + per_peer], (per_peer, per_peer)).T
            for c in range(height // per_peer):
                lanes = lax.broadcasted_iota(jnp.int32, (size, per_peer), 1) + c * per_peer
                pick_h[
                    d * room + top : d * room + top + size, c * per_peer : (c + 1) * per_peer
                ] = jnp.where(turned[:size, :] == lanes, 1.0, 0.0).astype(BF16)

    def rows_copy(phase, start, size, to, slot):
        return pltpu.make_async_remote_copy(
            src_ref=send_rows.at[to, pl.ds(start, size)],
            dst_ref=rows_in.at[slot, pl.ds(start, size)],
            send_sem=send_sem.at[phase, to],
            recv_sem=recv_sem.at[phase, slot],
            device_id={"dev": to},
            device_id_type=MESH,
        )

    def rows_for(to):
        rows = pl.ds(pl.multiple_of(to * room, 16), room)
        values = by_owner[...].reshape(n * cluster, breadth)
        return jnp.dot(pick_h[rows, :], values, preferred_element_type=F32).astype(BF16)

    def rows_out(off, carry):
        send_rows[peer(off)] = rows_for(peer(off))
        rows_copy(H_ONE, 0, early, peer(off), me).start()
        return carry

    lax.fori_loop(1, n, rows_out, 0)
    rows_in[me] = rows_for(me)

    for o in range(half):
        turned = jnp.broadcast_to(
            asked_h[beside(o), :, wide + 2 * per_peer :], (per_peer, per_peer)
        ).T
        for c in range(height // per_peer):
            lanes = lax.broadcasted_iota(jnp.int32, (depth, per_peer), 1) + c * per_peer
            pick_n[o * depth : (o + 1) * depth, c * per_peer : (c + 1) * per_peer] = jnp.where(
                turned[:depth, :] == lanes, 1.0, 0.0
            ).astype(BF16)

    def near_rows(to, at, slot):
        return pltpu.make_async_remote_copy(
            src_ref=send_near.at[at],
            dst_ref=mix.at[half + slot],
            send_sem=send_sem.at[NEAR_X, to],
            recv_sem=recv_sem.at[NEAR_X, side * half + slot],
            device_id={"dev": to},
            device_id_type=MESH,
        )

    moved_rows = jnp.dot(
        pick_n[...],
        send_x[...].reshape(n * cluster, breadth),
        preferred_element_type=F32,
    ).astype(BF16)
    mix[half + home] = moved_rows[:depth, :]
    for o in range(1, half):
        send_near[o] = moved_rows[o * depth : (o + 1) * depth, :]
        near_rows(beside(o), o, home).start()
    for o in range(half):
        mix[o, cross:, :] = jnp.zeros((depth - cross, breadth), BF16)
        turned = jnp.broadcast_to(seat_x[across(o)], (per_peer, per_peer)).T
        for c in range(n * depth // per_peer):
            lanes = lax.broadcasted_iota(jnp.int32, (per_peer, per_peer), 1) + c * per_peer
            place_x[o * per_peer : (o + 1) * per_peer, c * per_peer : (c + 1) * per_peer] = (
                jnp.where(turned == lanes.astype(F32), 1.0, 0.0).astype(BF16)
            )

    loads[5].wait()
    loads[6].wait()
    for i in range(height // tile):
        for j in range(pulled // tile):
            kept = occupancy[i, height // tile + j].astype(F32)
            rows, cols = pl.ds(i * tile, tile), pl.ds(j * tile, tile)
            part = (edge[rows, cols].astype(F32) * kept).astype(BF16)
            edge[rows, cols] = part
            edge_t[cols, rows] = part.T
    loads[7].wait()
    for i in range(height // tile):
        for j in range(height // tile):
            kept = occupancy[i, j].astype(F32)
            rows, cols = pl.ds(i * tile, tile), pl.ds(j * tile, tile)
            local[rows, cols] = (local[rows, cols].astype(F32) * kept).astype(BF16)

    receive(ASK, pulls, asked)
    for d in range(n):
        wanted = asked[d]
        rows = lax.broadcasted_iota(jnp.int32, (height, per_peer), 0)
        pick[:, d * per_peer : (d + 1) * per_peer] = jnp.where(rows == wanted, 1.0, 0.0).astype(
            BF16
        )
        listed = asked_h[d, :, wide + per_peer : wide + 2 * per_peer]
        turned = jnp.broadcast_to(listed, (per_peer, per_peer)).T
        lanes = lax.broadcasted_iota(jnp.int32, (per_peer, per_peer), 1)
        for c in range(height // per_peer):
            pick_t[d * per_peer : (d + 1) * per_peer, c * per_peer : (c + 1) * per_peer] = (
                jnp.where(turned == lanes + c * per_peer, 1.0, 0.0).astype(BF16)
            )

    def blocks_out(phase, left, right, src, dst):
        values = right[...].reshape(left.shape[1], breadth)

        def block(to):
            rows = pl.ds(pl.multiple_of(to * per_peer, per_peer), per_peer)
            return jnp.dot(left[rows, :], values, preferred_element_type=F32).astype(BF16)

        def one(off, carry):
            src[peer(off)] = block(peer(off))
            send(phase, src, dst, off)
            return carry

        lax.fori_loop(1, n, one, 0)
        dst[me] = block(me)

    def bands(body):
        def one(i, carry):
            body(pl.ds(pl.multiple_of(i * band, band), band))
            return carry

        lax.fori_loop(0, height // band, one, 0)

    def times(left, rows, right):
        values = right[...].reshape(left.shape[1], breadth)
        return jnp.dot(left[rows, :], values, preferred_element_type=F32)

    receive(MOVE_X, send_x, own_x)

    def cross_copy(to, slot):
        return pltpu.make_async_remote_copy(
            src_ref=send_far_x.at[to, pl.ds(0, cross)],
            dst_ref=mix.at[slot, pl.ds(0, cross)],
            send_sem=send_sem.at[FAR_X, to],
            recv_sem=recv_sem.at[FAR_X, (1 - side) * half + slot],
            device_id={"dev": to},
            device_id_type=MESH,
        )

    def cross_sent(to, slot):
        return pltpu.make_async_remote_copy(
            src_ref=send_far_x.at[to, pl.ds(0, cross)],
            dst_ref=mix.at[slot, pl.ds(0, cross)],
            send_sem=send_sem.at[FAR_X, to],
            recv_sem=recv_sem.at[FAR_X, side * half + slot],
            device_id={"dev": to},
            device_id_type=MESH,
        )

    def far_block(to):
        rows = pl.ds(pl.multiple_of(to * per_peer, per_peer), per_peer)
        values = own_x[...].reshape(height, breadth)
        return jnp.dot(pick_t[rows, :], values, preferred_element_type=F32).astype(BF16)

    def far_across(o, carry):
        to = across(o)
        send_far_x[to] = far_block(to)
        cross_sent(to, home).start()
        return carry

    def far_beside(o, carry):
        to = beside(o)
        send_far_x[to] = far_block(to)
        outgoing(FAR_X, send_far_x, far_x, to, me).start()
        return carry

    lax.fori_loop(0, half, far_across, 0)
    lax.fori_loop(1, half, far_beside, 0)
    far_x[me] = far_block(me)
    blocks_out(PUSH_ONE, edge_t, own_x, send_one, push_one)
    for off in range(1, n):
        rows_copy(H_TWO, early, room - early, peer(off), me).start()

    def local_one(rows):
        acc[rows, :] = times(local, rows, own_x)

    bands(local_one)
    for o in range(1, half):
        other = beside(o)
        outgoing(FAR_X, send_far_x, far_x, other, other).wait_recv()
        near_rows(other, o, lax.rem(home + o, half)).wait_recv()
    for o in range(half):
        cross_copy(across(o), lax.rem(home + o, half)).wait_recv()
    for o in range(half):
        far_x[across(o)] = jnp.dot(
            place_x[o * per_peer : (o + 1) * per_peer, :],
            mix[...].reshape(n * depth, breadth),
            preferred_element_type=F32,
        ).astype(BF16)

    def edge_one(rows):
        acc[rows, :] = acc[rows, :] + times(edge, rows, far_x)

    bands(edge_one)
    receive(PUSH_ONE, send_one, push_one)

    def first(rows):
        total = (acc[rows, :] + times(pick, rows, push_one)).astype(BF16)
        value = jnp.dot(total, w_first[...], preferred_element_type=F32) + bias_first[...]
        value = jnp.maximum(value, 0.0).astype(BF16)
        hidden[rows, :] = value

    loads[8].wait()
    loads[9].wait()
    bands(first)
    blocks_out(PUSH_TWO, edge_t, hidden, send_two, push_two)

    def local_two(rows):
        acc[rows, :] = times(local, rows, hidden)

    bands(local_two)
    for off in range(1, n):
        rows_copy(H_ONE, 0, early, peer(off), peer(off)).wait_recv()
    for off in range(1, n):
        rows_copy(H_TWO, early, room - early, peer(off), peer(off)).wait_recv()

    def gather_h(rows):
        far_h[rows, :] = times(place, rows, rows_in).astype(BF16)

    bands(gather_h)

    def edge_two(rows):
        acc[rows, :] = acc[rows, :] + times(edge, rows, far_h)

    bands(edge_two)
    loads[10].wait()
    loads[11].wait()
    for off in range(1, reps):
        flag_copy(rep_peer(off), rep_peer(off)).wait_recv()
    full = flag_all[0]
    for r in range(1, reps):
        full = jnp.maximum(full, flag_all[r])
    flag_out[0] = jnp.where(jnp.max(full.astype(F32)) > 0.5, 1, 0)
    receive(PUSH_TWO, send_two, push_two)

    def second(rows):
        agg[rows, :] = (acc[rows, :] + times(pick, rows, push_two)).astype(BF16)

    bands(second)
    grad = lax.dot_general(
        agg[...], cotangent[...], (((0,), (0,)), ((), ())), preferred_element_type=F32
    )
    grad_mine[...] = grad.reshape(grad_mine.shape).astype(BF16)

    def near_copy(phase, src, dst, to, slot):
        return pltpu.make_async_remote_copy(
            src_ref=src,
            dst_ref=dst.at[slot],
            send_sem=near_send.at[phase, to],
            recv_sem=near_recv.at[phase, slot],
            device_id=near_id(to),
            device_id_type=MESH,
        )

    def far_copy(to, slot):
        return pltpu.make_async_remote_copy(
            src_ref=strip_mine,
            dst_ref=strip_far.at[slot],
            send_sem=far_send.at[to],
            recv_sem=far_recv.at[slot],
            device_id=far_id(to),
            device_id_type=MESH,
        )

    for off in range(1, everyone):
        near_copy(0, grad_mine.at[near(off)], grad_near, near(off), spot).start()

    def last(rows):
        output_out[rows, :] = jnp.dot(
            agg[rows, :], w_second[...], preferred_element_type=F32
        ).astype(BF16)

    bands(last)
    total = grad_mine[spot].astype(F32)
    for off in range(1, everyone):
        near_copy(0, grad_mine.at[near(off)], grad_near, near(off), near(off)).wait_recv()
        total = total + grad_near[near(off)].astype(F32)
    strip_mine[...] = total.astype(BF16)
    for off in range(1, outer):
        far_copy(far(off), line).start()
    strip_far[line] = strip_mine[...]
    for off in range(1, outer):
        far_copy(far(off), far(off)).wait_recv()
    total = strip_far[0].astype(F32)
    for z in range(1, outer):
        total = total + strip_far[z].astype(F32)
    total_mine[...] = total.astype(BF16)
    for off in range(1, everyone):
        near_copy(1, total_mine, grad_all, near(off), spot).start()
    grad_all[spot] = total_mine[...]
    for off in range(1, everyone):
        near_copy(1, total_mine, grad_all, near(off), near(off)).wait_recv()
    grad_out[...] = grad_all[...].astype(F32).reshape(grad_out.shape)

    finish(ASK, pulls, asked)
    finish(MOVE_X, send_x, own_x)
    for o in range(half):
        cross_sent(across(o), home).wait_send()
    for o in range(1, half):
        outgoing(FAR_X, send_far_x, far_x, beside(o), me).wait_send()
        near_rows(beside(o), o, home).wait_send()
    finish(ASK_H, codes, asked_h)
    for off in range(1, n):
        rows_copy(H_ONE, 0, early, peer(off), me).wait_send()
        rows_copy(H_TWO, early, room - early, peer(off), me).wait_send()
    for off in range(1, reps):
        flag_copy(rep_peer(off), my_rep).wait_send()
    finish(PUSH_ONE, send_one, push_one)
    finish(PUSH_TWO, send_two, push_two)
    for off in range(1, everyone):
        near_copy(0, grad_mine.at[near(off)], grad_near, near(off), spot).wait_send()
        near_copy(1, total_mine, grad_all, near(off), spot).wait_send()
    for off in range(1, outer):
        far_copy(far(off), line).wait_send()


def store_kernel(count, *refs):
    sems = refs[-1]
    copies = [
        pltpu.make_async_copy(refs[i], refs[count + i], sems.at[i]) for i in range(count)
    ]
    for copy in copies:
        copy.start()
    for copy in copies:
        copy.wait()


def store(*values):
    count = len(values)
    return pl.pallas_call(
        functools.partial(store_kernel, count),
        out_shape=tuple(pltpu.HBM(v.shape, v.dtype) for v in values),
        in_specs=[pl.BlockSpec(memory_space=pltpu.VMEM)] * count,
        out_specs=tuple(pl.BlockSpec(memory_space=pl.ANY) for _ in values),
        scratch_shapes=[pltpu.SemaphoreType.DMA((count,))],
        compiler_params=pltpu.CompilerParams(vmem_limit_bytes=8 * 1024 * 1024),
    )(*values)


def fused(
    features,
    history,
    new_owner,
    pull_rows,
    occupancy,
    adj_local,
    adj_boundary,
    w_first,
    bias_first,
    w_second,
    cotangent,
):
    n, reps = lax.axis_size("dev"), lax.axis_size("rep")
    height, breadth = features.shape
    cluster = height // n
    pulled = pull_rows.shape[0]
    per_peer = pulled // n
    inner = near_width(n)
    everyone = inner * reps
    part = breadth // everyone
    vmem = pl.BlockSpec(memory_space=pltpu.VMEM)
    anywhere = pl.BlockSpec(memory_space=pltpu.HBM)
    moved = pltpu.VMEM((n, cluster, breadth), BF16)
    listed = pltpu.VMEM((n, per_peer, breadth), BF16)
    square = pltpu.VMEM((everyone, part, breadth), BF16)
    strip = pltpu.VMEM((part, breadth), BF16)
    weight = pltpu.VMEM((breadth, breadth), BF16)
    nodes = pltpu.VMEM((height, breadth), BF16)
    room = row_room(per_peer)
    wide = -(-room // 128) * 128
    asks = pltpu.VMEM((n, 1, wide + 3 * per_peer), jnp.int32)
    half = n // 2
    depth = near_rows_room(per_peer)
    rows = pltpu.VMEM((n, room, breadth), BF16)
    results = pl.pallas_call(
        functools.partial(step_kernel, n, reps, inner),
        out_shape=(
            pltpu.VMEM((height, breadth), BF16),
            pltpu.VMEM((height, breadth), BF16),
            pltpu.VMEM((breadth, breadth), F32),
            pltpu.SMEM((1,), jnp.int32),
        ),
        in_specs=[anywhere] * 12,
        out_specs=(vmem, vmem, vmem, pl.BlockSpec(memory_space=pltpu.SMEM)),
        scratch_shapes=[
            nodes,
            nodes,
            pltpu.SMEM(new_owner.shape, jnp.int32),
            pltpu.VMEM((n, 1, per_peer), jnp.int32),
            pltpu.VMEM((n, per_peer), jnp.int32),
            pltpu.SMEM(occupancy.shape, jnp.int32),
            weight,
            pltpu.VMEM((1, breadth), F32),
            weight,
            pltpu.VMEM((height, height), BF16),
            pltpu.VMEM((height, pulled), BF16),
            pltpu.VMEM((pulled, height), BF16),
            nodes,
            pltpu.VMEM((n, 1, per_peer), jnp.int32),
            asks,
            asks,
            pltpu.VMEM((height, pulled), BF16),
            pltpu.VMEM((pulled, height), BF16),
            pltpu.VMEM((n * room, height), BF16),
            pltpu.VMEM((pulled, n * room), BF16),
            pltpu.VMEM((half * depth, height), BF16),
            pltpu.VMEM((half * per_peer, n * depth), BF16),
            pltpu.VMEM((n, 1, per_peer), F32),
            moved,
            moved,
            moved,
            listed,
            rows,
            pltpu.VMEM((half, depth, breadth), BF16),
            listed,
            pltpu.VMEM((n, depth, breadth), BF16),
            rows,
            pltpu.VMEM((pulled, breadth), BF16),
            listed,
            listed,
            listed,
            listed,
            pltpu.VMEM((height, breadth), F32),
            nodes,
            square,
            square,
            strip,
            pltpu.VMEM((n // inner, part, breadth), BF16),
            strip,
            square,
            pltpu.VMEM((1, per_peer), jnp.int32),
            pltpu.VMEM((reps, 1, per_peer), jnp.int32),
            pltpu.SemaphoreType.DMA((12,)),
            pltpu.SemaphoreType.DMA((9, n)),
            pltpu.SemaphoreType.DMA((9, n)),
            pltpu.SemaphoreType.DMA((2, everyone)),
            pltpu.SemaphoreType.DMA((2, everyone)),
            pltpu.SemaphoreType.DMA((n // inner,)),
            pltpu.SemaphoreType.DMA((n // inner,)),
            pltpu.SemaphoreType.DMA((reps,)),
            pltpu.SemaphoreType.DMA((reps,)),
        ],
        compiler_params=pltpu.CompilerParams(
            collective_id=0, has_side_effects=True, vmem_limit_bytes=40 * 1024 * 1024
        ),
    )(
        *(
            pltpu.with_memory_space_constraint(value, pltpu.HBM)
            for value in (
                features,
                history,
                new_owner,
                pull_rows.reshape(n, 1, per_peer),
                pull_rows.reshape(n, per_peer),
                occupancy,
                adj_local,
                adj_boundary,
                w_first,
                bias_first.reshape(1, breadth),
                w_second,
                cotangent,
            )
        )
    )
    return results


def row_room(per_peer):
    return per_peer * 11 // 8


def near_rows_room(per_peer):
    return per_peer * 7 // 8


def cross_rows(per_peer):
    return per_peer * 3 // 4


def early_rows(room):
    return room // 32 * 16


def near_width(n):
    return 2 if n % 2 == 0 else 1


def fits(peers, height, pulled, breadth, reps):
    return (
        height % (128 * peers) == 0
        and pulled == 128 * peers
        and peers % 2 == 0
        and peers * row_room(128) % 128 == 0
        and peers * near_rows_room(128) % 128 == 0
        and breadth % (16 * near_width(peers) * reps) == 0
    )


def expand(occupied):
    return jnp.repeat(jnp.repeat(occupied, 128, axis=0), 128, axis=1).astype(jnp.bfloat16)


def dense_terms(owned, remote, adj_local, adj_boundary, occupancy):
    height = owned.shape[0]
    full_mask = expand(occupancy)
    local_tile = adj_local * full_mask[:, :height]
    edge_tile = adj_boundary * full_mask[:, height:]
    summed = jnp.dot(local_tile, owned, preferred_element_type=jnp.float32)
    summed = summed + jnp.dot(edge_tile, remote, preferred_element_type=jnp.float32)
    partial_value = lax.dot_general(
        edge_tile, owned, (((0,), (0,)), ((), ())), preferred_element_type=jnp.float32
    )
    return (summed, partial_value)


def body(*args):
    features, pull_rows = args[0], args[3]
    peer_count = lax.axis_size("dev")
    height, breadth = features.shape
    if not fits(peer_count, height, pull_rows.shape[0], breadth, lax.axis_size("rep")):
        return plain(*args)
    *results, full = fused(*args)
    return lax.cond(full[0] > 0, lambda: store(*plain(*args)), lambda: store(*results))


def plain(
    features,
    history,
    new_owner,
    pull_rows,
    occupancy,
    adj_local,
    adj_boundary,
    w_first,
    bias_first,
    w_second,
    cotangent,
):
    peer_count = lax.axis_size("dev")
    height, breadth = features.shape
    cluster = height // peer_count
    pulled = pull_rows.shape[0]
    per_peer = pulled // peer_count
    everyone = peer_count * lax.axis_size("rep")
    indices = jnp.arange(peer_count, dtype=jnp.int32)
    matches = (new_owner[0][:, None] == indices[None, :]).astype(jnp.int32)
    inverse = jnp.sum(matches * indices[:, None], axis=0)

    def arrange(values):
        return values.reshape(peer_count, cluster, breadth)[inverse]

    requests = lax.all_to_all(
        pull_rows.reshape(peer_count, per_peer), "dev", split_axis=0, concat_axis=0, tiled=True
    ).reshape(pulled)

    def fetch_rows(values):
        return values[requests].reshape(peer_count, per_peer, breadth)

    selector = (requests[None, :] == jnp.arange(height, dtype=jnp.int32)[:, None]).astype(
        jnp.bfloat16
    )

    def collect(received):
        return jnp.dot(
            selector, received.reshape(pulled, breadth), preferred_element_type=jnp.float32
        )

    def layer_terms(owned, remote):
        return dense_terms(owned, remote, adj_local, adj_boundary, occupancy)

    moved_x, moved_h = (
        lax.all_to_all(arrange(features), "dev", split_axis=0, concat_axis=0, tiled=True),
        lax.all_to_all(arrange(history), "dev", split_axis=0, concat_axis=0, tiled=True),
    )
    own_x = moved_x.reshape(height, breadth)
    own_h = moved_h.reshape(height, breadth)
    far_x, far_h = (
        lax.all_to_all(fetch_rows(own_x), "dev", split_axis=0, concat_axis=0, tiled=True),
        lax.all_to_all(fetch_rows(own_h), "dev", split_axis=0, concat_axis=0, tiled=True),
    )
    summed_one, partial_one = layer_terms(own_x, far_x.reshape(pulled, breadth))
    pushed_one = lax.all_to_all(
        partial_one.astype(jnp.bfloat16).reshape(peer_count, per_peer, breadth),
        "dev",
        split_axis=0,
        concat_axis=0,
        tiled=True,
    )
    far_h = far_h.reshape(pulled, breadth)
    aggregate_one = (summed_one + collect(pushed_one)).astype(jnp.bfloat16)
    hidden = jnp.maximum(
        jnp.dot(aggregate_one, w_first, preferred_element_type=jnp.float32) + bias_first, 0.0
    ).astype(jnp.bfloat16)
    summed_two, partial_two = layer_terms(hidden, far_h)
    pushed_two = lax.all_to_all(
        partial_two.astype(jnp.bfloat16).reshape(peer_count, per_peer, breadth),
        "dev",
        split_axis=0,
        concat_axis=0,
        tiled=True,
    )
    aggregate_two = (summed_two + collect(pushed_two)).astype(jnp.bfloat16)
    output = jnp.dot(aggregate_two, w_second, preferred_element_type=jnp.float32).astype(
        jnp.bfloat16
    )
    local_grad = lax.dot_general(
        aggregate_two, cotangent, (((0,), (0,)), ((), ())), preferred_element_type=jnp.float32
    )
    slices = lax.all_to_all(
        local_grad.reshape(everyone, breadth // everyone, breadth),
        ("dev", "rep"),
        split_axis=0,
        concat_axis=0,
        tiled=True,
    )
    gradient = lax.all_gather(jnp.sum(slices, axis=0), ("dev", "rep"), axis=0, tiled=True)
    return (hidden, output, gradient)


def solution(mesh):
    return jax.shard_map(
        body,
        mesh=mesh,
        in_specs=(
            P(("dev", "rep"), None),
            P(("dev", "rep"), None),
            P(("dev", "rep"), None),
            P(("dev", "rep")),
            P(("dev", "rep"), None),
            P(("dev", "rep"), None),
            P(("dev", "rep"), None),
            P(),
            P(),
            P(),
            P(("dev", "rep"), None),
        ),
        out_specs=(P(("dev", "rep"), None), P(("dev", "rep"), None), P()),
        check_vma=False,
    )
```

```python
import functools

import jax
import jax.numpy as jnp
from jax import lax
from jax.experimental import pallas as pl
from jax.experimental.pallas import tpu as pltpu
from jax.sharding import PartitionSpec as P

MESH = pl.DeviceIdType.MESH
F32 = jnp.float32
BF16 = jnp.bfloat16
ASK, ASK_H, MOVE_X, FAR_X, H_ONE, H_TWO, NEAR_X, FAR_B, PUSH_ONE, PUSH_TWO = range(10)


def step_kernel(
    n,
    reps,
    inner,
    features_hbm,
    history_hbm,
    new_owner_hbm,
    pulls_hbm,
    lists_hbm,
    occupancy_hbm,
    adj_local_hbm,
    adj_edge_hbm,
    w_first_hbm,
    bias_first_hbm,
    w_second_hbm,
    cotangent_hbm,
    hidden,
    output_out,
    grad_out,
    flag_out,
    features,
    history,
    new_owner,
    pulls,
    lists,
    occupancy,
    w_first,
    bias_first,
    w_second,
    local,
    edge,
    edge_t,
    cotangent,
    asked,
    codes,
    asked_h,
    pick,
    pick_t,
    pick_h,
    place,
    pick_n,
    place_x,
    seat_x,
    send_x,
    by_owner,
    own_x,
    send_far_x,
    send_rows,
    send_near,
    far_x,
    mix,
    rows_in,
    far_h,
    send_one,
    send_two,
    push_one,
    push_two,
    acc,
    agg,
    grad_mine,
    grad_near,
    strip_mine,
    strip_far,
    total_mine,
    grad_all,
    flag_mine,
    flag_all,
    load_sem,
    send_sem,
    recv_sem,
    near_send,
    near_recv,
    far_send,
    far_recv,
    flag_send,
    flag_recv,
):
    me = lax.axis_index("dev")
    my_rep = lax.axis_index("rep")
    height, breadth = features.shape
    cluster = height // n
    per_peer = pulls.shape[2]
    pulled = n * per_peer
    tile = height // occupancy.shape[0]
    band = min(256, height)
    room = send_rows.shape[1]
    early = early_rows(room)
    wide = codes.shape[2] - 3 * per_peer
    half = n // 2
    depth = mix.shape[1]
    cross = cross_rows(per_peer)
    home = lax.rem(me, half)
    side = me // half

    def beside(off):
        return side * half + lax.rem(home + off, half)

    def across(off):
        return (1 - side) * half + lax.rem(home + off, half)

    def peer(off):
        return lax.rem(me + off, n)

    def rep_peer(off):
        return lax.rem(my_rep + off, reps)

    everyone = inner * reps
    outer = n // inner
    line = me // inner
    spot = lax.rem(me, inner) * reps + my_rep

    def near(off):
        return lax.rem(spot + off, everyone)

    def near_id(at):
        return {"dev": line * inner + at // reps, "rep": lax.rem(at, reps)}

    def far(off):
        return lax.rem(line + off, outer)

    def far_id(at):
        return {"dev": at * inner + lax.rem(me, inner)}

    barrier = pltpu.get_barrier_semaphore()
    for off in range(1, n):
        pl.semaphore_signal(barrier, inc=1, device_id={"dev": peer(off)}, device_id_type=MESH)
    for lane in range(inner):
        for off in range(1, reps):
            pl.semaphore_signal(
                barrier,
                inc=1,
                device_id={
                    "dev": line * inner + lax.rem(me + lane, inner),
                    "rep": rep_peer(off),
                },
                device_id_type=MESH,
            )

    loads = [
        pltpu.make_async_copy(source, target, load_sem.at[i])
        for i, (source, target) in enumerate(
            (
                (new_owner_hbm, new_owner),
                (features_hbm, features),
                (lists_hbm, lists),
                (pulls_hbm, pulls),
                (history_hbm, history),
                (occupancy_hbm, occupancy),
                (adj_edge_hbm, edge),
                (adj_local_hbm, local),
                (w_first_hbm, w_first),
                (bias_first_hbm, bias_first),
                (w_second_hbm, w_second),
                (cotangent_hbm, cotangent),
            )
        )
    ]
    for load in loads:
        load.start()

    def cluster_for(source, owner):
        block = jnp.zeros((cluster, breadth), BF16)
        for j in range(n):
            chosen = jnp.where(new_owner[0, j] == owner, 1.0, 0.0)
            weight = jnp.full((cluster, breadth), chosen, F32).astype(BF16)
            block = block + source[j * cluster : (j + 1) * cluster, :] * weight
        return block

    def outgoing(phase, src, dst, to, slot):
        return pltpu.make_async_remote_copy(
            src_ref=src.at[to],
            dst_ref=dst.at[slot],
            send_sem=send_sem.at[phase],
            recv_sem=recv_sem.at[phase],
            device_id={"dev": to},
            device_id_type=MESH,
        )

    def bulk(piece, sent, arrived):
        return pltpu.make_async_remote_copy(
            src_ref=piece,
            dst_ref=piece,
            send_sem=sent,
            recv_sem=arrived,
            device_id={"dev": peer(1)},
            device_id_type=MESH,
        )

    def arrived(phase, piece):
        bulk(piece, send_sem.at[phase], recv_sem.at[phase]).wait_recv()

    def left(phase, piece):
        bulk(piece, send_sem.at[phase], recv_sem.at[phase]).wait_send()

    def send(phase, src, dst, off):
        outgoing(phase, src, dst, peer(off), me).start()

    def receive(phase, src, dst):
        arrived(phase, dst.at[pl.ds(0, n - 1)])

    def finish(phase, src, dst):
        left(phase, src.at[pl.ds(0, n - 1)])

    def slots():
        upper = jnp.where(
            lax.broadcasted_iota(jnp.int32, (per_peer, per_peer), 0)
            <= lax.broadcasted_iota(jnp.int32, (per_peer, per_peer), 1),
            1.0,
            0.0,
        ).astype(BF16)
        origin = lax.broadcasted_iota(jnp.int32, (n, per_peer), 0)
        seats = lax.broadcasted_iota(jnp.int32, (wide, per_peer), 0).astype(F32)
        held, within = [], []
        for e in range(n):
            row = jnp.broadcast_to(lists[e : e + 1, :], (n, per_peer)) - origin * cluster
            held.append(jnp.where((row >= 0) & (row < cluster), 1.0, 0.0))
            within.append(row.astype(F32))
        stacked = jnp.concatenate(held, axis=0).astype(BF16)
        prefix = jnp.dot(stacked, upper, preferred_element_type=F32)
        totals = jnp.dot(
            stacked, jnp.ones((per_peer, per_peer), BF16), preferred_element_type=F32
        )
        before = jnp.full((n, per_peer), -1.0, F32)
        over = jnp.zeros((n, per_peer), F32)
        table = jnp.zeros((2 * n, wide), F32)
        lanes = seats[:per_peer]
        away = (origin // half != side).astype(F32)
        nearby = 1.0 - away
        spot_s = lax.rem(origin, half) + half
        behind = jnp.full((n, per_peer), -1.0, F32)
        table_n = jnp.zeros((2 * n, per_peer), F32)
        places = []
        for e in range(n):
            remote = jnp.where(e // half != side, 1.0, 0.0)
            ahead = prefix[e * n : (e + 1) * n, :]
            rank = jnp.sum(ahead * away, axis=0, keepdims=True) - 1.0
            gone = held[e] * away
            stays = held[e] * nearby * remote
            seat = stays * (ahead + behind)
            behind = behind + remote * totals[e * n : (e + 1) * n, :]
            over = jnp.maximum(over, seat + float(room - depth))
            over = jnp.maximum(over, remote * gone * rank + float(room - cross))
            seat_x[e] = jnp.sum(
                seat
                + stays * (spot_s * depth).astype(F32)
                + gone * (rank + float(e % half * depth)),
                axis=0,
                keepdims=True,
            )
            taken = jnp.where(lanes == rank, 1.0, 0.0).astype(BF16)
            entry = jnp.concatenate([gone * origin.astype(F32), gone * within[e]], axis=0)
            listed = lax.dot_general(
                entry.astype(BF16), taken, (((1,), (1,)), ((), ())), preferred_element_type=F32
            )
            listed = jnp.sum(
                listed[:n, :] * float(cluster) + listed[n:, :], axis=0, keepdims=True
            ).astype(jnp.int32)
            codes[e, :, wide + per_peer : wide + 2 * per_peer] = jnp.where(
                e // half != side, listed, lists[e : e + 1, :]
            )
            mine = jnp.sum(seat, axis=0, keepdims=True)
            taken = jnp.where(lanes == mine, 1.0, 0.0).astype(BF16)
            entry = jnp.concatenate([stays * float(e), stays * within[e]], axis=0)
            table_n = table_n + lax.dot_general(
                entry.astype(BF16), taken, (((1,), (1,)), ((), ())), preferred_element_type=F32
            )
        for e in range(n):
            seat = held[e] * (prefix[e * n : (e + 1) * n, :] + before)
            before = before + totals[e * n : (e + 1) * n, :]
            over = jnp.maximum(over, seat)
            places.append(
                jnp.sum(seat + held[e] * (origin * room).astype(F32), axis=0, keepdims=True)
            )
            mine = jnp.sum(seat, axis=0, keepdims=True)
            taken = jnp.where(seats == mine, 1.0, 0.0).astype(BF16)
            entry = jnp.concatenate([held[e] * float(e), held[e] * within[e]], axis=0)
            table = table + lax.dot_general(
                entry.astype(BF16), taken, (((1,), (1,)), ((), ())), preferred_element_type=F32
            )
        found = (table[:n, :] * float(cluster) + table[n:, :]).astype(jnp.int32)
        full = jnp.where(jnp.max(over, axis=0, keepdims=True) >= float(room), 1, 0)
        found_n = (table_n[:n, :] * float(cluster) + table_n[n:, :]).astype(jnp.int32)
        for d in range(n):
            codes[d, :, :wide] = found[d : d + 1, :]
            codes[d, :, wide : wide + per_peer] = full
            codes[d, :, wide + 2 * per_peer :] = found_n[d : d + 1, :]
        return places

    loads[2].wait()
    places = slots()
    loads[0].wait()
    loads[1].wait()
    for off in range(1, n):
        send_x[peer(off)] = cluster_for(features, peer(off))
    own_x[me] = cluster_for(features, me)
    send_x[me] = own_x[me]
    loads[3].wait()
    pl.semaphore_wait(barrier, n - 1 + inner * (reps - 1))
    for off in range(1, n):
        send(ASK_H, codes, asked_h, off)
    for off in range(1, n):
        send(ASK, pulls, asked, off)
    for off in range(1, n):
        send(MOVE_X, send_x, own_x, off)
    asked[me] = pulls[me]
    asked_h[me] = codes[me]
    loads[4].wait()
    for e in range(n):
        by_owner[e] = cluster_for(history, e)
    for e in range(n):
        turned = jnp.broadcast_to(places[e], (per_peer, per_peer)).T
        for c in range(n * room // per_peer):
            lanes = lax.broadcasted_iota(jnp.int32, (per_peer, per_peer), 1) + c * per_peer
            place[e * per_peer : (e + 1) * per_peer, c * per_peer : (c + 1) * per_peer] = (
                jnp.where(turned == lanes.astype(F32), 1.0, 0.0).astype(BF16)
            )

    def flag_copy(to, slot):
        return pltpu.make_async_remote_copy(
            src_ref=flag_mine,
            dst_ref=flag_all.at[slot],
            send_sem=flag_send,
            recv_sem=flag_recv,
            device_id={"rep": to},
            device_id_type=MESH,
        )

    receive(ASK_H, codes, asked_h)
    full = asked_h[0, :, wide : wide + per_peer]
    for d in range(1, n):
        full = jnp.maximum(full, asked_h[d, :, wide : wide + per_peer])
    flag_mine[...] = full
    for off in range(1, reps):
        flag_copy(rep_peer(off), my_rep).start()
    flag_all[my_rep] = full
    for d in range(n):
        for top in range(0, room, per_peer):
            size = min(per_peer, room - top)
            turned = jnp.broadcast_to(asked_h[d, :, top : top + per_peer], (per_peer, per_peer)).T
            for c in range(height // per_peer):
                lanes = lax.broadcasted_iota(jnp.int32, (size, per_peer), 1) + c * per_peer
                pick_h[
                    d * room + top : d * room + top + size, c * per_peer : (c + 1) * per_peer
                ] = jnp.where(turned[:size, :] == lanes, 1.0, 0.0).astype(BF16)

    def rows_copy(phase, start, size, to, slot):
        return pltpu.make_async_remote_copy(
            src_ref=send_rows.at[to, pl.ds(start, size)],
            dst_ref=rows_in.at[slot, pl.ds(start, size)],
            send_sem=send_sem.at[phase],
            recv_sem=recv_sem.at[phase],
            device_id={"dev": to},
            device_id_type=MESH,
        )

    def rows_for(to):
        rows = pl.ds(pl.multiple_of(to * room, 16), room)
        values = by_owner[...].reshape(n * cluster, breadth)
        return jnp.dot(pick_h[rows, :], values, preferred_element_type=F32).astype(BF16)

    def rows_out(off, carry):
        send_rows[peer(off)] = rows_for(peer(off))
        rows_copy(H_ONE, 0, early, peer(off), me).start()
        return carry

    lax.fori_loop(1, n, rows_out, 0)
    rows_in[me] = rows_for(me)

    for o in range(half):
        turned = jnp.broadcast_to(
            asked_h[beside(o), :, wide + 2 * per_peer :], (per_peer, per_peer)
        ).T
        for c in range(height // per_peer):
            lanes = lax.broadcasted_iota(jnp.int32, (depth, per_peer), 1) + c * per_peer
            pick_n[o * depth : (o + 1) * depth, c * per_peer : (c + 1) * per_peer] = jnp.where(
                turned[:depth, :] == lanes, 1.0, 0.0
            ).astype(BF16)

    def near_rows(to, at, slot):
        return pltpu.make_async_remote_copy(
            src_ref=send_near.at[at],
            dst_ref=mix.at[half + slot],
            send_sem=send_sem.at[NEAR_X],
            recv_sem=recv_sem.at[NEAR_X],
            device_id={"dev": to},
            device_id_type=MESH,
        )

    moved_rows = jnp.dot(
        pick_n[...],
        send_x[...].reshape(n * cluster, breadth),
        preferred_element_type=F32,
    ).astype(BF16)
    mix[half + home] = moved_rows[:depth, :]
    for o in range(1, half):
        send_near[o] = moved_rows[o * depth : (o + 1) * depth, :]
        near_rows(beside(o), o, home).start()
    for o in range(half):
        mix[o, cross:, :] = jnp.zeros((depth - cross, breadth), BF16)
        turned = jnp.broadcast_to(seat_x[across(o)], (per_peer, per_peer)).T
        for c in range(n * depth // per_peer):
            lanes = lax.broadcasted_iota(jnp.int32, (per_peer, per_peer), 1) + c * per_peer
            place_x[o * per_peer : (o + 1) * per_peer, c * per_peer : (c + 1) * per_peer] = (
                jnp.where(turned == lanes.astype(F32), 1.0, 0.0).astype(BF16)
            )

    loads[5].wait()
    loads[6].wait()
    for i in range(height // tile):
        for j in range(pulled // tile):
            kept = occupancy[i, height // tile + j].astype(F32)
            rows, cols = pl.ds(i * tile, tile), pl.ds(j * tile, tile)
            part = (edge[rows, cols].astype(F32) * kept).astype(BF16)
            edge[rows, cols] = part
            edge_t[cols, rows] = part.T
    loads[7].wait()
    for i in range(height // tile):
        for j in range(height // tile):
            kept = occupancy[i, j].astype(F32)
            rows, cols = pl.ds(i * tile, tile), pl.ds(j * tile, tile)
            local[rows, cols] = (local[rows, cols].astype(F32) * kept).astype(BF16)

    receive(ASK, pulls, asked)
    for d in range(n):
        wanted = asked[d]
        rows = lax.broadcasted_iota(jnp.int32, (height, per_peer), 0)
        pick[:, d * per_peer : (d + 1) * per_peer] = jnp.where(rows == wanted, 1.0, 0.0).astype(
            BF16
        )
        listed = asked_h[d, :, wide + per_peer : wide + 2 * per_peer]
        turned = jnp.broadcast_to(listed, (per_peer, per_peer)).T
        lanes = lax.broadcasted_iota(jnp.int32, (per_peer, per_peer), 1)
        for c in range(height // per_peer):
            pick_t[d * per_peer : (d + 1) * per_peer, c * per_peer : (c + 1) * per_peer] = (
                jnp.where(turned == lanes + c * per_peer, 1.0, 0.0).astype(BF16)
            )

    def blocks_out(phase, left, right, src, dst):
        values = right[...].reshape(left.shape[1], breadth)

        def block(to):
            rows = pl.ds(pl.multiple_of(to * per_peer, per_peer), per_peer)
            return jnp.dot(left[rows, :], values, preferred_element_type=F32).astype(BF16)

        def one(off, carry):
            src[peer(off)] = block(peer(off))
            send(phase, src, dst, off)
            return carry

        lax.fori_loop(1, n, one, 0)
        dst[me] = block(me)

    def bands(body):
        def one(i, carry):
            body(pl.ds(pl.multiple_of(i * band, band), band))
            return carry

        lax.fori_loop(0, height // band, one, 0)

    def times(left, rows, right):
        values = right[...].reshape(left.shape[1], breadth)
        return jnp.dot(left[rows, :], values, preferred_element_type=F32)

    receive(MOVE_X, send_x, own_x)

    def cross_sent(to, slot):
        return pltpu.make_async_remote_copy(
            src_ref=send_far_x.at[to, pl.ds(0, cross)],
            dst_ref=mix.at[slot, pl.ds(0, cross)],
            send_sem=send_sem.at[FAR_X],
            recv_sem=recv_sem.at[FAR_X],
            device_id={"dev": to},
            device_id_type=MESH,
        )

    def far_block(to):
        rows = pl.ds(pl.multiple_of(to * per_peer, per_peer), per_peer)
        values = own_x[...].reshape(height, breadth)
        return jnp.dot(pick_t[rows, :], values, preferred_element_type=F32).astype(BF16)

    def far_across(o, carry):
        to = across(o)
        send_far_x[to] = far_block(to)
        cross_sent(to, home).start()
        return carry

    def far_beside(o, carry):
        to = beside(o)
        send_far_x[to] = far_block(to)
        outgoing(FAR_B, send_far_x, far_x, to, me).start()
        return carry

    lax.fori_loop(0, half, far_across, 0)
    lax.fori_loop(1, half, far_beside, 0)
    far_x[me] = far_block(me)
    blocks_out(PUSH_ONE, edge_t, own_x, send_one, push_one)
    for off in range(1, n):
        rows_copy(H_TWO, early, room - early, peer(off), me).start()

    def local_one(rows):
        acc[rows, :] = times(local, rows, own_x)

    bands(local_one)
    arrived(FAR_B, far_x.at[pl.ds(0, half - 1)])
    arrived(NEAR_X, mix.at[pl.ds(0, half - 1)])
    arrived(FAR_X, mix.at[pl.ds(0, half), pl.ds(0, cross)])
    for o in range(half):
        far_x[across(o)] = jnp.dot(
            place_x[o * per_peer : (o + 1) * per_peer, :],
            mix[...].reshape(n * depth, breadth),
            preferred_element_type=F32,
        ).astype(BF16)

    def edge_one(rows):
        acc[rows, :] = acc[rows, :] + times(edge, rows, far_x)

    bands(edge_one)
    receive(PUSH_ONE, send_one, push_one)

    def first(rows):
        total = (acc[rows, :] + times(pick, rows, push_one)).astype(BF16)
        value = jnp.dot(total, w_first[...], preferred_element_type=F32) + bias_first[...]
        value = jnp.maximum(value, 0.0).astype(BF16)
        hidden[rows, :] = value

    loads[8].wait()
    loads[9].wait()
    bands(first)
    blocks_out(PUSH_TWO, edge_t, hidden, send_two, push_two)

    def local_two(rows):
        acc[rows, :] = times(local, rows, hidden)

    bands(local_two)
    arrived(H_ONE, rows_in.at[pl.ds(0, n - 1), pl.ds(0, early)])
    arrived(H_TWO, rows_in.at[pl.ds(0, n - 1), pl.ds(early, room - early)])

    def gather_h(rows):
        far_h[rows, :] = times(place, rows, rows_in).astype(BF16)

    bands(gather_h)

    def edge_two(rows):
        acc[rows, :] = acc[rows, :] + times(edge, rows, far_h)

    bands(edge_two)
    loads[10].wait()
    loads[11].wait()
    if reps > 1:
        bulk(flag_all.at[pl.ds(0, reps - 1)], flag_send, flag_recv).wait_recv()
    full = flag_all[0]
    for r in range(1, reps):
        full = jnp.maximum(full, flag_all[r])
    flag_out[0] = jnp.where(jnp.max(full.astype(F32)) > 0.5, 1, 0)
    receive(PUSH_TWO, send_two, push_two)

    def second(rows):
        agg[rows, :] = (acc[rows, :] + times(pick, rows, push_two)).astype(BF16)

    bands(second)
    grad = lax.dot_general(
        agg[...], cotangent[...], (((0,), (0,)), ((), ())), preferred_element_type=F32
    )
    grad_mine[...] = grad.reshape(grad_mine.shape).astype(BF16)

    def near_copy(phase, src, dst, to, slot):
        return pltpu.make_async_remote_copy(
            src_ref=src,
            dst_ref=dst.at[slot],
            send_sem=near_send.at[phase],
            recv_sem=near_recv.at[phase],
            device_id=near_id(to),
            device_id_type=MESH,
        )

    def far_copy(to, slot):
        return pltpu.make_async_remote_copy(
            src_ref=strip_mine,
            dst_ref=strip_far.at[slot],
            send_sem=far_send,
            recv_sem=far_recv,
            device_id=far_id(to),
            device_id_type=MESH,
        )

    for off in range(1, everyone):
        near_copy(0, grad_mine.at[near(off)], grad_near, near(off), spot).start()

    def last(rows):
        output_out[rows, :] = jnp.dot(
            agg[rows, :], w_second[...], preferred_element_type=F32
        ).astype(BF16)

    bands(last)
    total = grad_mine[spot].astype(F32)
    bulk(grad_near.at[pl.ds(0, everyone - 1)], near_send.at[0], near_recv.at[0]).wait_recv()
    for off in range(1, everyone):
        total = total + grad_near[near(off)].astype(F32)
    strip_mine[...] = total.astype(BF16)
    for off in range(1, outer):
        far_copy(far(off), line).start()
    strip_far[line] = strip_mine[...]
    bulk(strip_far.at[pl.ds(0, outer - 1)], far_send, far_recv).wait_recv()
    total = strip_far[0].astype(F32)
    for z in range(1, outer):
        total = total + strip_far[z].astype(F32)
    total_mine[...] = total.astype(BF16)
    for off in range(1, everyone):
        near_copy(1, total_mine, grad_all, near(off), spot).start()
    grad_all[spot] = total_mine[...]
    bulk(grad_all.at[pl.ds(0, everyone - 1)], near_send.at[1], near_recv.at[1]).wait_recv()
    grad_out[...] = grad_all[...].astype(F32).reshape(grad_out.shape)

    finish(ASK, pulls, asked)
    finish(MOVE_X, send_x, own_x)
    left(FAR_X, send_far_x.at[pl.ds(0, half), pl.ds(0, cross)])
    left(FAR_B, send_far_x.at[pl.ds(0, half - 1)])
    left(NEAR_X, send_near.at[pl.ds(0, half - 1)])
    finish(ASK_H, codes, asked_h)
    left(H_ONE, send_rows.at[pl.ds(0, n - 1), pl.ds(0, early)])
    left(H_TWO, send_rows.at[pl.ds(0, n - 1), pl.ds(early, room - early)])
    if reps > 1:
        bulk(flag_all.at[pl.ds(0, reps - 1)], flag_send, flag_recv).wait_send()
    finish(PUSH_ONE, send_one, push_one)
    finish(PUSH_TWO, send_two, push_two)
    bulk(grad_near.at[pl.ds(0, everyone - 1)], near_send.at[0], near_recv.at[0]).wait_send()
    bulk(grad_all.at[pl.ds(0, everyone - 1)], near_send.at[1], near_recv.at[1]).wait_send()
    bulk(strip_far.at[pl.ds(0, outer - 1)], far_send, far_recv).wait_send()


def store_kernel(count, *refs):
    sems = refs[-1]
    copies = [
        pltpu.make_async_copy(refs[i], refs[count + i], sems.at[i]) for i in range(count)
    ]
    for copy in copies:
        copy.start()
    for copy in copies:
        copy.wait()


def store(*values):
    count = len(values)
    return pl.pallas_call(
        functools.partial(store_kernel, count),
        out_shape=tuple(pltpu.HBM(v.shape, v.dtype) for v in values),
        in_specs=[pl.BlockSpec(memory_space=pltpu.VMEM)] * count,
        out_specs=tuple(pl.BlockSpec(memory_space=pl.ANY) for _ in values),
        scratch_shapes=[pltpu.SemaphoreType.DMA((count,))],
        compiler_params=pltpu.CompilerParams(vmem_limit_bytes=8 * 1024 * 1024),
    )(*values)


def fused(
    features,
    history,
    new_owner,
    pull_rows,
    occupancy,
    adj_local,
    adj_boundary,
    w_first,
    bias_first,
    w_second,
    cotangent,
):
    n, reps = lax.axis_size("dev"), lax.axis_size("rep")
    height, breadth = features.shape
    cluster = height // n
    pulled = pull_rows.shape[0]
    per_peer = pulled // n
    inner = near_width(n)
    everyone = inner * reps
    part = breadth // everyone
    vmem = pl.BlockSpec(memory_space=pltpu.VMEM)
    anywhere = pl.BlockSpec(memory_space=pltpu.HBM)
    moved = pltpu.VMEM((n, cluster, breadth), BF16)
    listed = pltpu.VMEM((n, per_peer, breadth), BF16)
    square = pltpu.VMEM((everyone, part, breadth), BF16)
    strip = pltpu.VMEM((part, breadth), BF16)
    weight = pltpu.VMEM((breadth, breadth), BF16)
    nodes = pltpu.VMEM((height, breadth), BF16)
    room = row_room(per_peer)
    wide = -(-room // 128) * 128
    asks = pltpu.VMEM((n, 1, wide + 3 * per_peer), jnp.int32)
    half = n // 2
    depth = near_rows_room(per_peer)
    rows = pltpu.VMEM((n, room, breadth), BF16)
    results = pl.pallas_call(
        functools.partial(step_kernel, n, reps, inner),
        out_shape=(
            pltpu.VMEM((height, breadth), BF16),
            pltpu.VMEM((height, breadth), BF16),
            pltpu.VMEM((breadth, breadth), F32),
            pltpu.SMEM((1,), jnp.int32),
        ),
        in_specs=[anywhere] * 12,
        out_specs=(vmem, vmem, vmem, pl.BlockSpec(memory_space=pltpu.SMEM)),
        scratch_shapes=[
            nodes,
            nodes,
            pltpu.SMEM(new_owner.shape, jnp.int32),
            pltpu.VMEM((n, 1, per_peer), jnp.int32),
            pltpu.VMEM((n, per_peer), jnp.int32),
            pltpu.SMEM(occupancy.shape, jnp.int32),
            weight,
            pltpu.VMEM((1, breadth), F32),
            weight,
            pltpu.VMEM((height, height), BF16),
            pltpu.VMEM((height, pulled), BF16),
            pltpu.VMEM((pulled, height), BF16),
            nodes,
            pltpu.VMEM((n, 1, per_peer), jnp.int32),
            asks,
            asks,
            pltpu.VMEM((height, pulled), BF16),
            pltpu.VMEM((pulled, height), BF16),
            pltpu.VMEM((n * room, height), BF16),
            pltpu.VMEM((pulled, n * room), BF16),
            pltpu.VMEM((half * depth, height), BF16),
            pltpu.VMEM((half * per_peer, n * depth), BF16),
            pltpu.VMEM((n, 1, per_peer), F32),
            moved,
            moved,
            moved,
            listed,
            rows,
            pltpu.VMEM((half, depth, breadth), BF16),
            listed,
            pltpu.VMEM((n, depth, breadth), BF16),
            rows,
            pltpu.VMEM((pulled, breadth), BF16),
            listed,
            listed,
            listed,
            listed,
            pltpu.VMEM((height, breadth), F32),
            nodes,
            square,
            square,
            strip,
            pltpu.VMEM((n // inner, part, breadth), BF16),
            strip,
            square,
            pltpu.VMEM((1, per_peer), jnp.int32),
            pltpu.VMEM((reps, 1, per_peer), jnp.int32),
            pltpu.SemaphoreType.DMA((12,)),
            pltpu.SemaphoreType.DMA((10,)),
            pltpu.SemaphoreType.DMA((10,)),
            pltpu.SemaphoreType.DMA((2,)),
            pltpu.SemaphoreType.DMA((2,)),
            pltpu.SemaphoreType.DMA,
            pltpu.SemaphoreType.DMA,
            pltpu.SemaphoreType.DMA,
            pltpu.SemaphoreType.DMA,
        ],
        compiler_params=pltpu.CompilerParams(
            collective_id=0, has_side_effects=True, vmem_limit_bytes=40 * 1024 * 1024
        ),
    )(
        *(
            pltpu.with_memory_space_constraint(value, pltpu.HBM)
            for value in (
                features,
                history,
                new_owner,
                pull_rows.reshape(n, 1, per_peer),
                pull_rows.reshape(n, per_peer),
                occupancy,
                adj_local,
                adj_boundary,
                w_first,
                bias_first.reshape(1, breadth),
                w_second,
                cotangent,
            )
        )
    )
    return results


def row_room(per_peer):
    return per_peer * 11 // 8


def near_rows_room(per_peer):
    return per_peer * 7 // 8


def cross_rows(per_peer):
    return per_peer * 3 // 4


def early_rows(room):
    return room // 32 * 16


def near_width(n):
    return 2 if n % 2 == 0 else 1


def fits(peers, height, pulled, breadth, reps):
    return (
        height % (128 * peers) == 0
        and pulled == 128 * peers
        and peers % 2 == 0
        and peers * row_room(128) % 128 == 0
        and peers * near_rows_room(128) % 128 == 0
        and breadth % (16 * near_width(peers) * reps) == 0
    )


def expand(occupied):
    return jnp.repeat(jnp.repeat(occupied, 128, axis=0), 128, axis=1).astype(jnp.bfloat16)


def dense_terms(owned, remote, adj_local, adj_boundary, occupancy):
    height = owned.shape[0]
    full_mask = expand(occupancy)
    local_tile = adj_local * full_mask[:, :height]
    edge_tile = adj_boundary * full_mask[:, height:]
    summed = jnp.dot(local_tile, owned, preferred_element_type=jnp.float32)
    summed = summed + jnp.dot(edge_tile, remote, preferred_element_type=jnp.float32)
    partial_value = lax.dot_general(
        edge_tile, owned, (((0,), (0,)), ((), ())), preferred_element_type=jnp.float32
    )
    return (summed, partial_value)


def body(*args):
    features, pull_rows = args[0], args[3]
    peer_count = lax.axis_size("dev")
    height, breadth = features.shape
    if not fits(peer_count, height, pull_rows.shape[0], breadth, lax.axis_size("rep")):
        return plain(*args)
    *results, full = fused(*args)
    return lax.cond(full[0] > 0, lambda: store(*plain(*args)), lambda: store(*results))


def plain(
    features,
    history,
    new_owner,
    pull_rows,
    occupancy,
    adj_local,
    adj_boundary,
    w_first,
    bias_first,
    w_second,
    cotangent,
):
    peer_count = lax.axis_size("dev")
    height, breadth = features.shape
    cluster = height // peer_count
    pulled = pull_rows.shape[0]
    per_peer = pulled // peer_count
    everyone = peer_count * lax.axis_size("rep")
    indices = jnp.arange(peer_count, dtype=jnp.int32)
    matches = (new_owner[0][:, None] == indices[None, :]).astype(jnp.int32)
    inverse = jnp.sum(matches * indices[:, None], axis=0)

    def arrange(values):
        return values.reshape(peer_count, cluster, breadth)[inverse]

    requests = lax.all_to_all(
        pull_rows.reshape(peer_count, per_peer), "dev", split_axis=0, concat_axis=0, tiled=True
    ).reshape(pulled)

    def fetch_rows(values):
        return values[requests].reshape(peer_count, per_peer, breadth)

    selector = (requests[None, :] == jnp.arange(height, dtype=jnp.int32)[:, None]).astype(
        jnp.bfloat16
    )

    def collect(received):
        return jnp.dot(
            selector, received.reshape(pulled, breadth), preferred_element_type=jnp.float32
        )

    def layer_terms(owned, remote):
        return dense_terms(owned, remote, adj_local, adj_boundary, occupancy)

    moved_x, moved_h = (
        lax.all_to_all(arrange(features), "dev", split_axis=0, concat_axis=0, tiled=True),
        lax.all_to_all(arrange(history), "dev", split_axis=0, concat_axis=0, tiled=True),
    )
    own_x = moved_x.reshape(height, breadth)
    own_h = moved_h.reshape(height, breadth)
    far_x, far_h = (
        lax.all_to_all(fetch_rows(own_x), "dev", split_axis=0, concat_axis=0, tiled=True),
        lax.all_to_all(fetch_rows(own_h), "dev", split_axis=0, concat_axis=0, tiled=True),
    )
    summed_one, partial_one = layer_terms(own_x, far_x.reshape(pulled, breadth))
    pushed_one = lax.all_to_all(
        partial_one.astype(jnp.bfloat16).reshape(peer_count, per_peer, breadth),
        "dev",
        split_axis=0,
        concat_axis=0,
        tiled=True,
    )
    far_h = far_h.reshape(pulled, breadth)
    aggregate_one = (summed_one + collect(pushed_one)).astype(jnp.bfloat16)
    hidden = jnp.maximum(
        jnp.dot(aggregate_one, w_first, preferred_element_type=jnp.float32) + bias_first, 0.0
    ).astype(jnp.bfloat16)
    summed_two, partial_two = layer_terms(hidden, far_h)
    pushed_two = lax.all_to_all(
        partial_two.astype(jnp.bfloat16).reshape(peer_count, per_peer, breadth),
        "dev",
        split_axis=0,
        concat_axis=0,
        tiled=True,
    )
    aggregate_two = (summed_two + collect(pushed_two)).astype(jnp.bfloat16)
    output = jnp.dot(aggregate_two, w_second, preferred_element_type=jnp.float32).astype(
        jnp.bfloat16
    )
    local_grad = lax.dot_general(
        aggregate_two, cotangent, (((0,), (0,)), ((), ())), preferred_element_type=jnp.float32
    )
    slices = lax.all_to_all(
        local_grad.reshape(everyone, breadth // everyone, breadth),
        ("dev", "rep"),
        split_axis=0,
        concat_axis=0,
        tiled=True,
    )
    gradient = lax.all_gather(jnp.sum(slices, axis=0), ("dev", "rep"), axis=0, tiled=True)
    return (hidden, output, gradient)


def solution(mesh):
    return jax.shard_map(
        body,
        mesh=mesh,
        in_specs=(
            P(("dev", "rep"), None),
            P(("dev", "rep"), None),
            P(("dev", "rep"), None),
            P(("dev", "rep")),
            P(("dev", "rep"), None),
            P(("dev", "rep"), None),
            P(("dev", "rep"), None),
            P(),
            P(),
            P(),
            P(("dev", "rep"), None),
        ),
        out_specs=(P(("dev", "rep"), None), P(("dev", "rep"), None), P()),
        check_vma=False,
    )
```
